32 devices in a mesh: mem: 4 (over x, core), ty: 2 (over y), tx: 4 (over z).
Axes of the slice: x: 2, y: 2, z: 4, core: 2. Of those that a mesh axis runs over, the one named last changes fastest.
Arguments:
- pressure: float32 [8, 50, 64, 512], P('mem', None, 'ty', 'tx'), may hold values from -6 to 6
- east_wind: float32 [8, 50, 64, 512], P('mem', None, 'ty', 'tx'), may hold values from -6 to 6
- north_wind: float32 [8, 50, 64, 512], P('mem', None, 'ty', 'tx'), may hold values from -6 to 6
- vertical_wind: float32 [8, 49, 64, 512], P('mem', None, 'ty', 'tx'), may hold values from -6 to 6
- sound_squared: float32 [50, 64, 512], P(None, 'ty', 'tx'), may hold values from 0.5 to 2
- thickness: float32 [50], replicated, may hold values from 0.05 to 0.5
- owner_map: int32 [8], replicated, may hold values from 0 to 7, each once
Outputs:
- analysis: float32 [2, 4, 6, 32, 128], P('ty', 'tx', None, 'mem')
The draws below stay inside these ranges and needn't reach their ends.
Inputs may be any that keep to these rules, and one draw needn't show every extreme that they name: `owner_map`: every tile index appears exactly once.
All inputs are finite; a program needn't handle non-finite values.
Results may differ from the reference program's by a relative error of at most 0.0001.
Values sent between devices are 32-bit elements; how exact they have to be, the bound alone decides.
A program may use at most 128 MiB of HBM per device.

```python
import math
import jax
import jax.numpy as jnp
from jax import lax

CY = 32
CX = 128
NZ = 50
SUBSTEPS = 2
MEMBERS = 8
NY = 64
NX = 512
WLEVELS = 49
TILES = 8
N_TY = 2
N_TX = 4


def levels(stream_key, dims, split, smallest, largest):
    def one(axis_at, parts):
        draws = jax.random.uniform(jax.random.fold_in(jax.random.fold_in(stream_key, 6), axis_at), (parts,), jnp.float32, smallest / len(split), largest / len(split))
        return jnp.repeat(jnp.exp(draws), dims[axis_at] // parts).reshape((-1,) + (1,) * (len(dims) - axis_at - 1))

    loudness = one(*split[0])
    for cut in split[1:]:
        loudness = loudness * one(*cut)
    return loudness


def noise(rng, shape, scale, most, pieces=(), held_as=jnp.bfloat16):
    array = jax.random.normal(rng, shape, jnp.float32) * scale
    if len(pieces) > 0:
        array = levels(rng, shape, pieces, -0.22, 0.18) * array
    return jnp.clip(array, min=-most, max=most).astype(held_as)


def setup_inputs(seed: int = 0) -> dict:
    key_list = jax.random.split(jax.random.key(seed), 8)
    return {
        "pressure": noise(key_list[0], (MEMBERS, NZ, NY, NX), 1.0, 6.0, ((0, 4), (2, 2), (3, 4)), jnp.float32),
        "east_wind": noise(key_list[1], (MEMBERS, NZ, NY, NX), 1.0, 6.0, ((0, 4), (2, 2), (3, 4)), jnp.float32),
        "north_wind": noise(key_list[2], (MEMBERS, NZ, NY, NX), 1.0, 6.0, ((0, 4), (2, 2), (3, 4)), jnp.float32),
        "vertical_wind": noise(key_list[3], (MEMBERS, WLEVELS, NY, NX), 1.0, 6.0, ((0, 4), (2, 2), (3, 4)), jnp.float32),
        "sound_squared": jnp.clip(jnp.exp(math.log(2.0) - 1.3862944 * jax.random.uniform(key_list[4], (NZ, NY, NX), jnp.float32) ** levels(key_list[4], (NZ, NY, NX), ((1, 2), (2, 4)), -0.2, 0.2)), 0.5, 2.0),
        "thickness": jnp.clip(jnp.exp(jax.random.uniform(key_list[5], (NZ,), jnp.float32, math.log(0.05), math.log(0.5))), 0.05, 0.5),
        "owner_map": jax.random.permutation(key_list[6], TILES).astype(jnp.int32),
    }


horiz_ratio = 0.35
vert_ratio = 1.5


def column_solve(coeff, rhs_list):
    count = len(rhs_list)
    factors = []
    values = []
    pivot = 1.0 + coeff[1] + coeff[0]
    values.append(rhs_list[0] / pivot)
    factors.append(-coeff[1] / pivot)
    for position in range(1, count):
        pivot = (1.0 + coeff[position + 1] + coeff[position]) + coeff[position] * factors[position - 1]
        values.append((rhs_list[position] + coeff[position] * values[position - 1]) / pivot)
        factors.append(-coeff[position + 1] / pivot)
    solved = [values[count - 1]]
    for position in range(count - 2, -1, -1):
        solved.insert(0, values[position] - factors[position] * solved[0])
    return solved


def member_run(pressure, east_wind, north_wind, vertical_wind, sound_squared, thickness):
    coeff_field = vert_ratio * vert_ratio * sound_squared
    coeff = [coeff_field[level] for level in range(NZ)]
    for substep in range(SUBSTEPS):
        east_wind = east_wind - horiz_ratio * (pressure - jnp.roll(pressure, 1, axis=2))
        north_wind = north_wind - horiz_ratio * (pressure - jnp.roll(pressure, 1, axis=1))
        divergence = (jnp.roll(east_wind, -1, axis=2) - east_wind) + (jnp.roll(north_wind, -1, axis=1) - north_wind)
        partial_value = pressure - horiz_ratio * sound_squared * divergence
        rhs_list = [vertical_wind[level] - vert_ratio * (partial_value[level + 1] - partial_value[level]) for level in range(NZ - 1)]
        vertical_wind = jnp.stack(column_solve(coeff, rhs_list), axis=0)
        zero_layer = jnp.zeros_like(partial_value[:1])
        padded = jnp.concatenate([zero_layer, vertical_wind, zero_layer], axis=0)
        pressure = partial_value - vert_ratio * sound_squared * (padded[1:] - padded[:-1])
    mass = jnp.einsum('k,kyx->yx', thickness, pressure, precision=lax.Precision.HIGHEST)
    east_total = jnp.einsum('k,kyx->yx', thickness, east_wind, precision=lax.Precision.HIGHEST)
    north_total = jnp.einsum('k,kyx->yx', thickness, north_wind, precision=lax.Precision.HIGHEST)
    return jnp.stack([mass, east_total, north_total], axis=0)


def reference(pressure, east_wind, north_wind, vertical_wind, sound_squared, thickness, owner_map):
    def one_member(fields):
        return member_run(fields[0], fields[1], fields[2], fields[3], sound_squared, thickness)

    integrals = lax.map(one_member, (pressure, east_wind, north_wind, vertical_wind))
    mean = jnp.sum(integrals, axis=0) / MEMBERS
    variance = jnp.sum((integrals - mean) ** 2, axis=0) / (MEMBERS - 1)
    stats = jnp.concatenate([mean, variance], axis=0)
    tiled = stats.reshape(6, N_TY, CY, N_TX, CX).transpose(1, 3, 0, 2, 4).reshape(N_TY * N_TX, 6, CY, CX)
    placed = jnp.zeros_like(tiled).at[owner_map.astype(jnp.int32)].set(tiled)
    return placed.reshape(N_TY, N_TX, 6, CY, CX)
```

```python
import functools

import jax
import jax.numpy as jnp
from jax import lax
from jax.experimental import pallas as pl
from jax.experimental.pallas import tpu as pltpu
from jax.sharding import PartitionSpec as P

SUBSTEPS = 2
MESH = pl.DeviceIdType.MESH

horiz_ratio = 0.35
vert_ratio = 1.5


def unrolled(count, body, carry, most=7):
    width = max(d for d in range(1, most + 1) if count % d == 0)

    def block(i, c):
        for j in range(width):
            c = body(i * width + j, c)
        return c

    return lax.fori_loop(0, count // width, block, carry)


def kernel(
    sizes,
    p_hbm, u_hbm, v_hbm, w_hbm, s_hbm, thick_hbm, owner_hbm,
    out,
    p, u, v, w, s, inv, g, lam, sig, alpha, edge_cols, edge_rows,
    csend, crecv, rsend, rrecv, ueast, vnorth,
    integ, gath, everyone, thick, owner,
    load_sem, small_sem, cs_sem, cr_sem, rs_sem, rr_sem, ms_sem, mr_sem, as_sem, ar_sem,
):
    n_mem, n_ty, n_tx = sizes
    own, levels, rows, cols = p.shape
    quarter = rows // n_mem
    tiles = n_ty * n_tx
    mem, ty, tx = lax.axis_index("mem"), lax.axis_index("ty"), lax.axis_index("tx")
    me = ty * n_tx + tx
    east, west = {"tx": lax.rem(tx + 1, n_tx)}, {"tx": lax.rem(tx + n_tx - 1, n_tx)}
    north, south = {"ty": lax.rem(ty + 1, n_ty)}, {"ty": lax.rem(ty + n_ty - 1, n_ty)}
    lane = lax.broadcasted_iota(jnp.int32, (rows, cols), 1)
    row = lax.broadcasted_iota(jnp.int32, (rows, cols), 0)
    zero = jnp.zeros((rows, cols), jnp.float32)
    lane8 = lax.broadcasted_iota(jnp.int32, (8, cols), 1)
    zero8 = jnp.zeros((8, cols), jnp.float32)

    def load(src, dst, sem):
        copy = pltpu.make_async_copy(src, dst, load_sem.at[sem])
        copy.start()
        return copy

    small = [
        pltpu.make_async_copy(thick_hbm, thick, small_sem.at[0]),
        pltpu.make_async_copy(owner_hbm, owner, small_sem.at[1]),
    ]
    for copy in small:
        copy.start()
    loads = {}
    for m in range(own):
        for i, (name, src, dst) in enumerate((("p", p_hbm, p), ("u", u_hbm, u), ("v", v_hbm, v))):
            loads[name, m] = load(src.at[m], dst.at[m], 4 * m + i)
    loads["s"] = load(s_hbm, s, 4 * own)
    for m in range(own):
        loads["w", m] = load(w_hbm.at[m], w.at[m], 4 * m + 3)

    barrier = pltpu.get_barrier_semaphore()

    far = lambda d: -(min(d[0], n_ty - d[0]) + min(d[1], n_tx - d[1]))
    offsets = sorted([(a, b) for a in range(n_ty) for b in range(n_tx)], key=far)

    def tile_id(i):
        a, b = offsets[i - 1]
        other_ty, other_tx = lax.rem(ty + a, n_ty), lax.rem(tx + b, n_tx)
        return other_ty * n_tx + other_tx, {"ty": other_ty, "tx": other_tx}

    def mem_id(i):
        other = lax.rem(mem + i, n_mem)
        return other, {"mem": other}

    for i in range(1, tiles):
        pl.semaphore_signal(barrier, inc=1, device_id=tile_id(i)[1], device_id_type=MESH)
    for i in range(1, n_mem):
        pl.semaphore_signal(barrier, inc=1, device_id=mem_id(i)[1], device_id_type=MESH)

    def remote(src, dst, ssem, rsem, where):
        return pltpu.make_async_remote_copy(
            src_ref=src, dst_ref=dst, send_sem=ssem, recv_sem=rsem, device_id=where, device_id_type=MESH
        )

    def halo_copies(sub, m):
        kinds = ((0, east, north), (1, west, south))
        copies = []
        for kind, across, along in kinds:
            copies.append(remote(
                rsend.at[sub, m, kind], rrecv.at[sub, m, kind],
                rs_sem.at[sub, m, kind], rr_sem.at[sub, m, kind], along))
            copies.append(remote(
                csend.at[sub, m, kind], crecv.at[sub, m, kind],
                cs_sem.at[sub, m, kind], cr_sem.at[sub, m, kind], across))
        return copies

    def pack_first(k, x, packed):
        return jnp.where(lane == cols - 1 - k, pltpu.roll(x, cols - 1 - k, 1), packed)

    def pack_last(k, x, packed):
        shift = cols - k if not isinstance(k, int) or k > 0 else 0
        return jnp.where(lane == cols - 1 - k, pltpu.roll(x, shift, 1), packed)

    def pack_inputs(m):
        def one(k, c):
            last, first = c
            pk = p[m, k]
            first = pack_first(k, u[m, k] - horiz_ratio * pk, first)
            last = jnp.where(lane == cols - 1 - k, pltpu.roll(pk, lax.rem(cols - k, cols), 1), last)
            rsend[0, m, 0, pl.ds(k, 1), :] = p[m, k, rows - 1 : rows, :]
            rsend[0, m, 1, pl.ds(k, 1), :] = v[m, k, 0:1, :] - horiz_ratio * p[m, k, 0:1, :]
            return last, first

        packs = unrolled(levels, one, (zero, zero), 5)
        for kind in range(2):
            csend[0, m, kind] = packs[kind]

    def pivots():
        def one(i, c):
            k = i + 1
            below, gprev, mass_below, value = c
            sk = s[k]
            b = (vert_ratio * vert_ratio) * sk
            mass = thick[k] * sk
            r = 1.0 / (1.0 + b + below - below * gprev)
            gk = b * r
            value = (vert_ratio * (mass - mass_below) + below * value) * r
            inv[k] = r
            g[k] = gk
            lam[k] = value
            return b, gk, mass, value

        unrolled(levels - 1, one, ((vert_ratio * vert_ratio) * s[0], zero, thick[0] * s[0], zero))

        def weights(k, here, above, first, last, mass):
            mu = thick[k] - vert_ratio * (here - above)
            sk = (horiz_ratio * horiz_ratio) * mu * s[k]
            sig[k] = sk
            alpha[k] = mu - 4.0 * sk
            edge_rows[0, pl.ds(k, 1), :] = sk[0:1, :]
            edge_rows[1, pl.ds(k, 1), :] = sk[rows - 1 : rows, :]
            edge_rows[2, pl.ds(k, 1), :] = jnp.zeros((1, cols), jnp.float32) + thick[k]
            mass = jnp.where(lane8 == cols - 1 - k, thick[k], mass)
            return pack_first(k, sk, first), pack_last(k, sk, last), mass

        def two(i, c):
            k = levels - 1 - i
            here = lam[k] + g[k] * c[0]
            lam[k] = here
            return (here,) + weights(k, here, *c)

        c = unrolled(levels - 1, two, (zero, zero, zero, zero8))
        first, last, mass = weights(0, zero, *c)
        edge_cols[0] = first
        edge_cols[1] = last
        edge_cols[2] = jnp.concatenate([mass] * (rows // 8), axis=0)

    def forward(m):
        ueast[m] = crecv[0, m, 1] + horiz_ratio * csend[0, m, 0]
        vnorth[m] = rrecv[0, m, 1] + horiz_ratio * rsend[0, m, 0]

        def level(k, usum, vsum, dsum):
            pk = p[m, k]
            pw = jnp.where(lane == 0, pltpu.roll(crecv[0, m, 0], k + 1, 1), pltpu.roll(pk, 1, 1))
            ps = jnp.where(row == 0, rrecv[0, m, 0, pl.ds(k, 1), :], pltpu.roll(pk, 1, 0))
            uk = u[m, k] - horiz_ratio * (pk - pw)
            vk = v[m, k] - horiz_ratio * (pk - ps)
            ue = jnp.where(lane == cols - 1, pltpu.roll(ueast[m], k, 1), pltpu.roll(uk, cols - 1, 1))
            vn = jnp.where(row == rows - 1, vnorth[m, pl.ds(k, 1), :], pltpu.roll(vk, rows - 1, 0))
            div = (ue - uk) + (vn - vk)
            part = pk - horiz_ratio * s[k] * div
            p[m, k] = part
            return part, usum + thick[k] * uk, vsum + thick[k] * vk, dsum + sig[k] * div

        def one(i, c):
            k = i + 1
            part_below, value = c[:2]
            part, *sums = level(k, *c[2:])
            rhs = w[m, i] - vert_ratio * (part - part_below)
            value = (rhs + (vert_ratio * vert_ratio) * s[i] * value) * inv[k]
            w[m, i] = value
            return (part, value, *sums)

        part, *sums = level(0, zero, zero, zero)
        return unrolled(levels - 1, one, (part, zero, *sums))[2:]

    def backward(m):
        def finish(k, pk, last, first):
            p[m, k] = pk
            rsend[1, m, 0, pl.ds(k, 1), :] = pk[rows - 1 : rows, :]
            rsend[1, m, 1, pl.ds(k, 1), :] = pk[0:1, :]
            return pack_last(k, pk, last), pack_first(k, pk, first)

        def one(i, c):
            k = levels - 1 - i
            above = c[0]
            here = w[m, k - 1] + g[k] * above
            w[m, k - 1] = here
            pk = p[m, k] - vert_ratio * s[k] * (above - here)
            return (here,) + finish(k, pk, c[1], c[2])

        c = unrolled(levels - 1, one, (zero,) * 3)
        last, first = finish(0, p[m, 0] - vert_ratio * s[0] * c[0], c[1], c[2])
        csend[1, m, 0] = last
        csend[1, m, 1] = first

    def weigh(m):
        def level(k, mass, total):
            pk = p[m, k]
            around = (pltpu.roll(pk, 1, 1) + pltpu.roll(pk, cols - 1, 1)) + (
                pltpu.roll(pk, 1, 0) + pltpu.roll(pk, rows - 1, 0))
            return mass + thick[k] * pk, total + (alpha[k] * pk + sig[k] * around)

        def one(i, c):
            mass, total = level(i + 1, *c)
            return mass, total + lam[i + 1] * w[m, i]

        return unrolled(levels - 1, one, level(0, zero, zero))

    def integrals(m, usum, vsum, dsum, mass, total):
        across = lambda x: jnp.sum(x, axis=1, keepdims=True)
        along = lambda x: jnp.sum(x, axis=0, keepdims=True)
        pw, ps = crecv[1, m, 0], rrecv[1, m, 0]
        total = total - dsum / horiz_ratio
        total = total + jnp.where(lane == 0, across(edge_cols[0] * (pw - csend[1, m, 0])), 0.0)
        total = total + jnp.where(
            lane == cols - 1, across(edge_cols[1] * (crecv[1, m, 1] - csend[1, m, 1])), 0.0)
        total = total + jnp.where(row == 0, along(edge_rows[0] * (ps - rsend[1, m, 0])), 0.0)
        total = total + jnp.where(
            row == rows - 1, along(edge_rows[1] * (rrecv[1, m, 1] - rsend[1, m, 1])), 0.0)
        mass_west = jnp.where(lane == 0, across(edge_cols[2] * pw), pltpu.roll(mass, 1, 1))
        mass_south = jnp.where(row == 0, along(edge_rows[2] * ps), pltpu.roll(mass, 1, 0))
        return (
            total,
            usum - horiz_ratio * (mass - mass_west),
            vsum - horiz_ratio * (mass - mass_south),
        )

    sent = []

    def send_halos(sub, m):
        for copy in halo_copies(sub, m):
            copy.start()
            sent.append(copy)

    for m in range(own):
        for name in "puv":
            loads[name, m].wait()
        pack_inputs(m)
        if m == 0:
            pl.semaphore_wait(barrier, tiles - 1 + n_mem - 1)
        send_halos(0, m)
    loads["s"].wait()
    for copy in small:
        copy.wait()
    pivots()

    sums = []
    for m in range(own):
        loads["w", m].wait()
        for copy in halo_copies(0, m):
            copy.wait_recv()
        sums.append(forward(m))
        backward(m)
        send_halos(1, m)
    sums = [(*sums[m], *weigh(m)) for m in range(own)]
    for m in range(own):
        for copy in halo_copies(1, m):
            copy.wait_recv()
        for f, total in enumerate(integrals(m, *sums[m])):
            for q in range(n_mem):
                integ[m, q, f] = total[q * quarter : (q + 1) * quarter]
        for i in range(1, n_mem):
            other, where = mem_id(i)
            copy = remote(
                integ.at[m, other], gath.at[mem, m], ms_sem.at[m, other], mr_sem.at[m, mem], where)
            copy.start()
            sent.append(copy)

    fields = [[integ[m, mem, f] for f in range(3)] for m in range(own)]
    for m in range(own):
        for i in range(1, n_mem):
            other, where = mem_id(i)
            remote(integ.at[m, other], gath.at[other, m], ms_sem.at[m, other], mr_sem.at[m, other], where).wait_recv()
            fields.append([gath[other, m, f] for f in range(3)])
    members = len(fields)
    for f in range(3):
        total = fields[0][f]
        for one in fields[1:]:
            total = total + one[f]
        mean = total / members
        second = (fields[0][f] - mean) ** 2
        for one in fields[1:]:
            second = second + (one[f] - mean) ** 2
        everyone[me, f] = mean
        everyone[me, 3 + f] = second / (members - 1)

    for i in range(1, tiles):
        other, where = tile_id(i)
        copy = remote(everyone.at[me], everyone.at[me], as_sem.at[i], ar_sem.at[me], where)
        copy.start()
        sent.append(copy)
    mine = jnp.int32(0)
    for t in range(tiles):
        mine = jnp.where(owner[t] == me, t, mine)
    for i in range(1, tiles):
        other, where = tile_id(i)
        remote(everyone.at[me], everyone.at[other], as_sem.at[i], ar_sem.at[other], where).wait_recv()
    out[0, 0] = everyone[mine]
    for copy in sent:
        copy.wait_send()


def solution(mesh):
    n_mem, n_ty, n_tx = (mesh.shape[a] for a in ("mem", "ty", "tx"))
    tiles = n_ty * n_tx

    def local(pressure, east_wind, north_wind, vertical_wind, sound_squared, thickness, owner_map):
        own, levels, rows, cols = pressure.shape
        quarter = rows // n_mem
        f32 = jnp.float32
        dma = pltpu.SemaphoreType.DMA
        anywhere = pl.BlockSpec(memory_space=pl.ANY)
        return pl.pallas_call(
            functools.partial(kernel, (n_mem, n_ty, n_tx)),
            name="acoustic",
            out_shape=pltpu.VMEM((1, 1, 6, quarter, cols), f32),
            in_specs=[anywhere] * 7,
            out_specs=pl.BlockSpec(memory_space=pltpu.VMEM),
            scratch_shapes=[
                pltpu.VMEM((own, levels, rows, cols), f32),
                pltpu.VMEM((own, levels, rows, cols), f32),
                pltpu.VMEM((own, levels, rows, cols), f32),
                pltpu.VMEM((own, levels - 1, rows, cols), f32),
                *[pltpu.VMEM((levels, rows, cols), f32)] * 6,
                pltpu.VMEM((3, rows, cols), f32),
                pltpu.VMEM((3, levels, cols), f32),
                pltpu.VMEM((SUBSTEPS, own, 2, rows, cols), f32),
                pltpu.VMEM((SUBSTEPS, own, 2, rows, cols), f32),
                pltpu.VMEM((SUBSTEPS, own, 2, levels, cols), f32),
                pltpu.VMEM((SUBSTEPS, own, 2, levels, cols), f32),
                pltpu.VMEM((own, rows, cols), f32),
                pltpu.VMEM((own, levels, cols), f32),
                pltpu.VMEM((own, n_mem, 3, quarter, cols), f32),
                pltpu.VMEM((n_mem, own, 3, quarter, cols), f32),
                pltpu.VMEM((tiles, 6, quarter, cols), f32),
                pltpu.SMEM(thickness.shape, f32),
                pltpu.SMEM(owner_map.shape, jnp.int32),
                dma((4 * own + 1,)),
                dma((2,)),
                dma((SUBSTEPS, own, 2)),
                dma((SUBSTEPS, own, 2)),
                dma((SUBSTEPS, own, 2)),
                dma((SUBSTEPS, own, 2)),
                dma((own, n_mem)),
                dma((own, n_mem)),
                dma((tiles,)),
                dma((tiles,)),
            ],
            compiler_params=pltpu.CompilerParams(collective_id=0, has_side_effects=True),
        )(pressure, east_wind, north_wind, vertical_wind, sound_squared, thickness, owner_map)

    field = P("mem", None, "ty", "tx")
    return jax.shard_map(
        local,
        mesh=mesh,
        in_specs=(field, field, field, field, P(None, "ty", "tx"), P(), P()),
        out_specs=P("ty", "tx", None, "mem", None),
        check_vma=False,
    )
```

```python
import functools

import jax
import jax.numpy as jnp
from jax import lax
from jax.experimental import pallas as pl
from jax.experimental.pallas import tpu as pltpu
from jax.sharding import PartitionSpec as P

MESH = pl.DeviceIdType.MESH
PAD = 8

horiz_ratio = 0.35
vert_ratio = 1.5


def unrolled(count, body, carry, most=7):
    width = max(d for d in range(1, most + 1) if count % d == 0)

    def block(i, c):
        for j in range(width):
            c = body(i * width + j, c)
        return c

    return lax.fori_loop(0, count // width, block, carry)


def kernel(
    sizes,
    p_hbm, u_hbm, v_hbm, w_hbm, s_hbm, thick_hbm, owner_hbm,
    out,
    p, u, v, w, s, part, hs, vs, inv, binv, g, lam, mu, alpha, sig, sig_east, sig_west,
    edge, edge_recv, first_row, row_recv, sig_edge, sig_edge_recv, sig_rows, p_edge, p_rows,
    integ, gath, rim, rim_recv, lip, lip_recv, everyone, thick, owner,
    load_sem, small_sem, send_sem, member_sem, recv_sem,
):
    n_mem, n_ty, n_tx = sizes
    own, levels, rows, cols = u.shape
    quarter = rows // n_mem
    tiles = n_ty * n_tx
    body = pl.ds(PAD, rows)
    mem, ty, tx = lax.axis_index("mem"), lax.axis_index("ty"), lax.axis_index("tx")
    me = ty * n_tx + tx
    east, west = lax.rem(tx + 1, n_tx), lax.rem(tx + n_tx - 1, n_tx)
    north, south = lax.rem(ty + 1, n_ty), lax.rem(ty + n_ty - 1, n_ty)
    scope = jax.named_scope

    greet = {(i, 0, 0) for i in range(n_mem)} | {(0, a, b) for a in range(n_ty) for b in range(n_tx)}
    for i in range(n_mem):
        greet |= {(i, 0, 1 % n_tx), (i, 0, (n_tx - 1) % n_tx), (i, 1 % n_ty, 0), (i, (n_ty - 1) % n_ty, 0)}
    greet = sorted(greet - {(0, 0, 0)})
    barrier = pltpu.get_barrier_semaphore()
    for i, a, b in greet:
        where = {"mem": lax.rem(mem + i, n_mem), "ty": lax.rem(ty + a, n_ty), "tx": lax.rem(tx + b, n_tx)}
        pl.semaphore_signal(barrier, inc=1, device_id=where, device_id_type=MESH)

    def load(src, dst, sem):
        copy = pltpu.make_async_copy(src, dst, sem)
        copy.start()
        return copy

    loads = {}
    for m in range(own):
        loads["p", m] = load(p_hbm.at[m], p.at[m, :, body, :], load_sem.at[3 * m])
        loads["u", m] = load(u_hbm.at[m], u.at[m], load_sem.at[3 * m + 1])
        loads["v", m] = load(v_hbm.at[m], v.at[m, :, pl.ds(0, rows), :], load_sem.at[3 * m + 2])
        if m == 0:
            small = [load(thick_hbm, thick, small_sem.at[0]), load(owner_hbm, owner, small_sem.at[1])]
    loads["s"] = load(s_hbm, s, load_sem.at[3 * own])
    loads["w"] = load(w_hbm, w, load_sem.at[3 * own + 1])

    lane = lax.broadcasted_iota(jnp.int32, (rows, cols), 1)
    row = lax.broadcasted_iota(jnp.int32, (rows, cols), 0)
    lane8 = lax.broadcasted_iota(jnp.int32, (8, cols), 1)
    row8 = lax.broadcasted_iota(jnp.int32, (8, cols), 0)
    pair = lane >> 1
    even = (lane & 1) == 0
    is_first, is_last = lane == 0, lane == cols - 1
    is_edge = is_first | is_last
    zero = jnp.zeros((rows, cols), jnp.float32)
    blank = jnp.zeros((1, cols), jnp.float32)

    def to_west(x):
        return pltpu.roll(x, cols - 1, 1)

    def to_east(x):
        return pltpu.roll(x, 1, 1)

    def drain(ref, sem):
        pltpu.make_async_copy(ref, ref, sem).wait()

    def send(src, dst, kind, sem, where):
        pltpu.make_async_remote_copy(
            src_ref=src, dst_ref=dst, send_sem=send_sem.at[kind], recv_sem=sem, device_id=where, device_id_type=MESH
        ).start()

    def clear(k, c):
        for m in range(own):
            p[m, k, PAD - 1 : PAD, :] = blank
            p[m, k, PAD + rows : PAD + rows + 1, :] = blank
            v[m, k, rows : rows + 1, :] = blank
        sig[k, PAD - 1 : PAD, :] = blank
        sig[k, PAD + rows : PAD + rows + 1, :] = blank
        return c

    def pack(m):
        def one(k, packed):
            pk = p[m, k, body, :]
            ends = jnp.where(is_last, pk, u[m, k] - horiz_ratio * pk)
            first_row[m, pl.ds(k, 1), :] = v[m, k, 0:1, :] - horiz_ratio * p[m, k, PAD : PAD + 1, :]
            return jnp.where(pair == k, pltpu.roll(ends, 2 * k + 1, 1), packed)

        edge[m] = unrolled(levels, one, zero, 25)

    def pivots():
        def one(i, c):
            k = i + 1
            below, gprev, mass_below, value = c
            sk = s[k]
            hs[k] = horiz_ratio * sk
            vs[k] = vert_ratio * sk
            b = (vert_ratio * vert_ratio) * sk
            mass = thick[k] * sk
            r = 1.0 / (1.0 + b + below - below * gprev)
            gk = b * r
            bi = below * r
            value = (vert_ratio * (mass - mass_below)) * r + bi * value
            inv[k] = r
            binv[k] = bi
            g[k] = gk
            lam[k] = value
            return b, gk, mass, value

        s0 = s[0]
        hs[0] = horiz_ratio * s0
        vs[0] = vert_ratio * s0
        unrolled(levels - 1, one, ((vert_ratio * vert_ratio) * s0, zero, thick[0] * s0, zero))

        def weights(k, here, above, packed):
            mk = thick[k] - vert_ratio * (here - above)
            sk = (horiz_ratio * mk) * hs[k]
            mu[k] = mk
            sig[k, body, :] = sk
            sig_east[k] = to_west(sk)
            sig_west[k] = to_east(sk)
            alpha[k] = mk - 4.0 * sk
            return jnp.where(pair == k, pltpu.roll(sk, 2 * k + 1, 1), packed)

        def two(i, c):
            k = levels - 1 - i
            above, packed = c
            here = lam[k] + g[k] * above
            lam[k] = here
            return here, weights(k, here, above, packed)

        above, packed = unrolled(levels - 1, two, (zero, zero))
        sig_edge[...] = weights(0, zero, above, packed)

    def diverge(m):
        def one(k, c):
            usum, vsum, psum = c
            pk, uk, vk = p[m, k, body, :], u[m, k], v[m, k, pl.ds(0, rows), :]
            around = to_east(pk) + (p[m, k, pl.ds(PAD - 1, rows), :] + p[m, k, pl.ds(PAD + 1, rows), :])
            div = (to_west(uk - horiz_ratio * pk) - uk) + (v[m, k, pl.ds(1, rows), :] - vk)
            u[m, k] = div - horiz_ratio * (around - 4.0 * pk)
            tk = thick[k]
            return usum + tk * uk, vsum + tk * vk, psum + tk * pk

        return unrolled(levels, one, (zero, zero, zero), 10)

    def forward(m):
        mine = edge[m]
        halo = jnp.where(
            even, -horiz_ratio * (edge_recv[m, 0] - mine), pltpu.roll(edge_recv[m, 1] - mine, cols - 2, 1))

        def level(k, rest):
            hk = pltpu.roll(halo, lax.rem(cols - 2 * k, cols), 1)
            div = u[m, k] + jnp.where(is_edge, hk, 0.0)
            low = jnp.where(row8 == 0, -horiz_ratio * row_recv[m, 0, pl.ds(k, 1), :], 0.0)
            high = jnp.where(row8 == 7, row_recv[m, 1, pl.ds(k, 1), :], 0.0)
            div = jnp.concatenate([div[:8] + low, div[8 : rows - 8], div[rows - 8 :] + high], axis=0)
            e = hs[k] * div
            pa = p[m, k, body, :] - e
            part[m, k] = pa
            return pa, rest - mu[k] * e

        def one(i, c):
            k = i + 1
            pa_below, value, rest = c
            pa, rest = level(k, rest)
            rhs = w[m, i] - vert_ratio * (pa - pa_below)
            value = rhs * inv[k] + binv[k] * value
            w[m, i] = value
            return pa, value, rest

        pa, rest = level(0, zero)
        return unrolled(levels - 1, one, (pa, zero, rest))[2]

    def backward(m, rest):
        def weigh(k, pk, packed, mass, rest, te, tw, tn, ts):
            p_rows[m, 0, pl.ds(k, 1), :] = pk[0:1]
            p_rows[m, 1, pl.ds(k, 1), :] = pk[rows - 1 : rows]
            return (
                jnp.where(pair == k, pltpu.roll(pk, 2 * k + 1, 1), packed),
                mass + thick[k] * pk,
                rest + alpha[k] * pk,
                te + sig_east[k] * pk,
                tw + sig_west[k] * pk,
                tn + sig[k, pl.ds(PAD + 1, rows), :] * pk,
                ts + sig[k, pl.ds(PAD - 1, rows), :] * pk,
            )

        def one(i, c):
            k = levels - 1 - i
            above, packed, mass, rest, *sides = c
            here = w[m, k - 1] + g[k] * above
            pk = part[m, k] - vs[k] * (above - here)
            return (here, *weigh(k, pk, packed, mass, rest + lam[k] * here, *sides))

        above, *sums = unrolled(levels - 1, one, (zero, zero, zero, rest, zero, zero, zero, zero))
        packed, *sums = weigh(0, part[m, 0] - vs[0] * above, *sums)
        p_edge[m] = packed
        return sums

    def whole(m, usum, vsum, q, rest, te, tw, tn, ts):
        total = rest + jnp.where(is_first, 0.0, to_east(te)) + jnp.where(is_last, 0.0, to_west(tw))
        total = total + pltpu.roll(tn, 1, 0) + pltpu.roll(ts, rows - 1, 0)
        ue = usum - horiz_ratio * (q - jnp.where(is_first, 0.0, to_east(q)))
        vn = vsum - horiz_ratio * (q - jnp.where(row == 0, 0.0, pltpu.roll(q, 1, 0)))
        for r in range(n_mem):
            for f, x in enumerate((total, ue, vn)):
                integ[m, r, f] = x[r * quarter : (r + 1) * quarter]
        for i in range(1, n_mem):
            other = lax.rem(mem + i, n_mem)
            send(integ.at[m, other], gath.at[mem, m], 4, recv_sem.at[2], {"mem": other})

    def rims(qs):
        sig_e, sig_w = pltpu.roll(sig_edge_recv[1], cols - 1, 1), pltpu.roll(sig_edge_recv[0], 1, 1)
        rims = zero
        for m in range(own):
            te = jnp.sum(jnp.where(even, sig_e * p_edge[m], 0.0), axis=1, keepdims=True)
            tw = jnp.sum(jnp.where(even, 0.0, sig_w * p_edge[m]), axis=1, keepdims=True)
            rims = jnp.where(lane == 2 * m, te, rims)
            rims = jnp.where(lane == 2 * m + 1, pltpu.roll(qs[m], 2 * m + 2, 1), rims)
            rims = jnp.where(lane == cols - 1 - m, tw, rims)
        for r in range(n_mem):
            rim[r] = rims[r * quarter : (r + 1) * quarter]
        for i in range(n_mem):
            other = lax.rem(mem + i, n_mem)
            send(rim.at[other], rim_recv.at[0, mem], 5, recv_sem.at[3], {"mem": other, "tx": east})
            send(rim.at[other], rim_recv.at[1, mem], 5, recv_sem.at[3], {"mem": other, "tx": west})

    def lips(qs):
        for m in range(own):
            lip[m : m + 1, :] = jnp.sum(sig_rows[0] * p_rows[m, 1], axis=0, keepdims=True)
            lip[own + m : own + m + 1, :] = qs[m][rows - 1 : rows]
            lip[2 * own + m : 2 * own + m + 1, :] = jnp.sum(sig_rows[1] * p_rows[m, 0], axis=0, keepdims=True)
        send(lip, lip_recv.at[0, mem], 6, recv_sem.at[4], {"mem": 0, "ty": north})
        send(lip, lip_recv.at[1, mem], 6, recv_sem.at[4], {"mem": n_mem - 1, "ty": south})

    with scope("clear"):
        unrolled(levels, clear, 0, 10)
    for m in range(own):
        with scope(f"wait_load{m}"):
            for name in "puv":
                loads[name, m].wait()
        with scope(f"pack{m}"):
            pack(m)
    with scope("wait_barrier"):
        pl.semaphore_wait(barrier, len(greet))
    with scope("send"):
        for m in range(own):
            send(p.at[m, :, PAD + rows - 1, :], row_recv.at[m, 0], 0, member_sem.at[m, 0], {"ty": north})
            send(first_row.at[m], row_recv.at[m, 1], 0, member_sem.at[m, 0], {"ty": south})
            send(edge.at[m], edge_recv.at[m, 0], 1, member_sem.at[m, 1], {"tx": east})
            send(edge.at[m], edge_recv.at[m, 1], 1, member_sem.at[m, 1], {"tx": west})
    with scope("wait_s"):
        loads["s"].wait()
        for copy in small:
            copy.wait()
    with scope("pivots"):
        pivots()
    with scope("send_sig"):
        send(sig_edge, sig_edge_recv.at[0], 2, recv_sem.at[0], {"tx": east})
        send(sig_edge, sig_edge_recv.at[1], 2, recv_sem.at[0], {"tx": west})
        send(sig.at[:, PAD, :], sig_rows.at[0], 3, recv_sem.at[1], {"ty": south})
        send(sig.at[:, PAD + rows - 1, :], sig_rows.at[1], 3, recv_sem.at[1], {"ty": north})
    sums = []
    for m in range(own):
        with scope(f"diverge{m}"):
            sums.append(diverge(m))

    qs = []
    for m in range(own):
        with scope(f"wait_edge{m}"):
            if m == 0:
                loads["w"].wait()
            drain(edge_recv.at[m], member_sem.at[m, 1])
        with scope(f"wait_row{m}"):
            drain(row_recv.at[m], member_sem.at[m, 0])
        with scope(f"forward{m}"):
            rest = forward(m)
        with scope(f"backward{m}"):
            mass, *rest = backward(m, rest)
        qs.append(sums[m][2] + mass)
        if m == own - 1:
            with scope("wait_sig"):
                drain(sig_edge_recv, recv_sem.at[0])
            with scope("rims"):
                rims(qs)
        with scope(f"whole{m}"):
            whole(m, sums[m][0], sums[m][1], qs[m], *rest)
    with scope("wait_sig_rows"):
        drain(sig_rows, recv_sem.at[1])
    with scope("lips"):
        lips(qs)

    bottom = (row8[:quarter] == 0) & (mem == 0)
    top = (row8[:quarter] == quarter - 1) & (mem == n_mem - 1)
    with scope("wait_lip"):

        @pl.when((mem == 0) | (mem == n_mem - 1))
        def _():
            drain(lip_recv.at[0], recv_sem.at[4])

    with scope("wait_rim"):
        drain(rim_recv, recv_sem.at[3])
    with scope("wait_mem"):
        drain(gath.at[pl.ds(0, n_mem - 1)], recv_sem.at[2])

    with scope("stats"):
        fields = []
        lane_q = lane[:quarter]
        for i in range(n_mem):
            other = lax.rem(mem + i, n_mem)
            from_west, from_east = rim_recv[0, other], rim_recv[1, other]
            from_south, from_north = lip_recv[0, other], lip_recv[1, other]
            for m in range(own):
                source = integ.at[m, mem] if i == 0 else gath.at[other, m]
                total, ue, vn = (source[f] for f in range(3))
                te = from_west if m == 0 else pltpu.roll(from_west, cols - 2 * m, 1)
                tw = from_east if m == 0 else pltpu.roll(from_east, m, 1)
                total = total + jnp.where(lane_q == 0, te, 0.0) + jnp.where(lane_q == cols - 1, tw, 0.0)
                total = total + jnp.where(bottom, from_south[m : m + 1], 0.0)
                total = total + jnp.where(top, from_north[2 * own + m : 2 * own + m + 1], 0.0)
                ue = ue + horiz_ratio * jnp.where(lane_q == 0, pltpu.roll(from_west, cols - 2 * m - 1, 1), 0.0)
                vn = vn + horiz_ratio * jnp.where(bottom, from_south[own + m : own + m + 1], 0.0)
                fields.append([total, ue, vn])

        members = len(fields)
        for f in range(3):
            total = fields[0][f]
            for one in fields[1:]:
                total = total + one[f]
            mean = total / members
            second = (fields[0][f] - mean) ** 2
            for one in fields[1:]:
                second = second + (one[f] - mean) ** 2
            everyone[me, f] = mean
            everyone[me, 3 + f] = second / (members - 1)

        far = lambda d: -(min(d[0], n_ty - d[0]) + min(d[1], n_tx - d[1]))
        offsets = sorted([(a, b) for a in range(n_ty) for b in range(n_tx)], key=far)[:-1]
        for a, b in offsets:
            where = {"ty": lax.rem(ty + a, n_ty), "tx": lax.rem(tx + b, n_tx)}
            send(everyone.at[me], everyone.at[me], 7, recv_sem.at[5], where)
    mine = jnp.int32(0)
    for t in range(tiles):
        mine = jnp.where(owner[t] == me, t, mine)
    with scope("wait_all"):
        drain(everyone.at[pl.ds(0, tiles - 1)], recv_sem.at[5])
    with scope("finish"):
        out[0, 0] = everyone[mine]
        drain(row_recv, send_sem.at[0])
        drain(edge_recv, send_sem.at[1])
        drain(sig_edge_recv, send_sem.at[2])
        drain(sig_rows, send_sem.at[3])
        drain(gath.at[pl.ds(0, n_mem - 1)], send_sem.at[4])
        drain(rim_recv, send_sem.at[5])
        drain(lip_recv.at[0, pl.ds(0, 2)], send_sem.at[6])
        drain(everyone.at[pl.ds(0, tiles - 1)], send_sem.at[7])


def solution(mesh):
    n_mem, n_ty, n_tx = (mesh.shape[a] for a in ("mem", "ty", "tx"))
    tiles = n_ty * n_tx

    def local(pressure, east_wind, north_wind, vertical_wind, sound_squared, thickness, owner_map):
        own, levels, rows, cols = pressure.shape
        quarter = rows // n_mem
        f32 = jnp.float32
        dma = pltpu.SemaphoreType.DMA

        def vmem(*shape):
            return pltpu.VMEM(shape, f32)

        return pl.pallas_call(
            functools.partial(kernel, (n_mem, n_ty, n_tx)),
            name="acoustic",
            out_shape=pltpu.VMEM((1, 1, 6, quarter, cols), f32),
            in_specs=[pl.BlockSpec(memory_space=pl.ANY)] * 7,
            out_specs=pl.BlockSpec(memory_space=pltpu.VMEM),
            scratch_shapes=[
                vmem(own, levels, rows + 2 * PAD, cols),
                vmem(own, levels, rows, cols),
                vmem(own, levels, rows + PAD, cols),
                vmem(own, levels - 1, rows, cols),
                vmem(levels, rows, cols),
                vmem(own, levels, rows, cols),
                *[vmem(levels, rows, cols)] * 8,
                vmem(levels, rows + 2 * PAD, cols),
                *[vmem(levels, rows, cols)] * 2,
                vmem(own, rows, cols),
                vmem(own, 2, rows, cols),
                vmem(own, levels, cols),
                vmem(own, 2, levels, cols),
                vmem(rows, cols),
                vmem(2, rows, cols),
                vmem(2, levels, cols),
                vmem(own, rows, cols),
                vmem(own, 2, levels, cols),
                vmem(own, n_mem, 3, quarter, cols),
                vmem(n_mem, own, 3, quarter, cols),
                vmem(n_mem, quarter, cols),
                vmem(2, n_mem, quarter, cols),
                vmem(-(-3 * own // 8) * 8, cols),
                vmem(2, n_mem, -(-3 * own // 8) * 8, cols),
                vmem(tiles, 6, quarter, cols),
                pltpu.SMEM(thickness.shape, f32),
                pltpu.SMEM(owner_map.shape, jnp.int32),
                dma((3 * own + 2,)),
                dma((2,)),
                dma((8,)),
                dma((own, 2)),
                dma((6,)),
            ],
            compiler_params=pltpu.CompilerParams(collective_id=0, has_side_effects=True),
        )(pressure, east_wind, north_wind, vertical_wind, sound_squared, thickness, owner_map)

    field = P("mem", None, "ty", "tx")
    return jax.shard_map(
        local,
        mesh=mesh,
        in_specs=(field, field, field, field, P(None, "ty", "tx"), P(), P()),
        out_specs=P("ty", "tx", None, "mem", None),
        check_vma=False,
    )
```

```python
import functools

import jax
import jax.numpy as jnp
from jax import lax
from jax.experimental import pallas as pl
from jax.experimental.pallas import tpu as pltpu
from jax.sharding import PartitionSpec as P

MESH = pl.DeviceIdType.MESH
PAD = 8

horiz_ratio = 0.35
vert_ratio = 1.5


def unrolled(count, body, carry, most=7):
    trips = -(-count // most)
    width = count // trips
    first = count - trips * width

    def block(i, c):
        for j in range(width):
            c = body(first + i * width + j, c)
        return c

    for i in range(first):
        carry = body(i, carry)
    return lax.fori_loop(0, trips, block, carry)


def kernel(
    sizes,
    p_hbm, u_hbm, v_hbm, w_hbm, s_hbm, thick_hbm, owner_hbm,
    out,
    p, u, v, w, s, part, hs, vs, inv, binv, g, lam, mu, alpha, sig, sig_east, sig_west,
    edge, edge_recv, first_row, row_recv, sig_edge, sig_edge_recv, sig_rows, p_edge, p_rows,
    integ, gath, rim, rim_recv, lip, lip_recv, everyone, thick, owner,
    load_sem, small_sem, send_sem, member_sem, recv_sem,
):
    n_mem, n_ty, n_tx = sizes
    own, levels, rows, cols = u.shape
    quarter = rows // n_mem
    tiles = n_ty * n_tx
    body = pl.ds(PAD, rows)
    mem, ty, tx = lax.axis_index("mem"), lax.axis_index("ty"), lax.axis_index("tx")
    me = ty * n_tx + tx
    east, west = lax.rem(tx + 1, n_tx), lax.rem(tx + n_tx - 1, n_tx)
    north, south = lax.rem(ty + 1, n_ty), lax.rem(ty + n_ty - 1, n_ty)
    scope = jax.named_scope

    greet = {(i, 0, 0) for i in range(n_mem)} | {(0, a, b) for a in range(n_ty) for b in range(n_tx)}
    for i in range(n_mem):
        greet |= {(i, 0, 1 % n_tx), (i, 0, (n_tx - 1) % n_tx), (i, 1 % n_ty, 0), (i, (n_ty - 1) % n_ty, 0)}
    greet = sorted(greet - {(0, 0, 0)})
    barrier = pltpu.get_barrier_semaphore()
    for i, a, b in greet:
        where = {"mem": lax.rem(mem + i, n_mem), "ty": lax.rem(ty + a, n_ty), "tx": lax.rem(tx + b, n_tx)}
        pl.semaphore_signal(barrier, inc=1, device_id=where, device_id_type=MESH)

    def load(src, dst, sem):
        copy = pltpu.make_async_copy(src, dst, sem)
        copy.start()
        return copy

    loads = {"s": load(s_hbm, s, load_sem.at[3 * own])}
    small = [load(thick_hbm, thick, small_sem.at[0]), load(owner_hbm, owner, small_sem.at[1])]
    for m in range(own):
        loads["p", m] = load(p_hbm.at[m], p.at[m, :, body, :], load_sem.at[3 * m])
        loads["u", m] = load(u_hbm.at[m], u.at[m], load_sem.at[3 * m + 1])
        loads["v", m] = load(v_hbm.at[m], v.at[m, :, pl.ds(0, rows), :], load_sem.at[3 * m + 2])
    loads["w"] = load(w_hbm, w, load_sem.at[3 * own + 1])

    lane = lax.broadcasted_iota(jnp.int32, (rows, cols), 1)
    row = lax.broadcasted_iota(jnp.int32, (rows, cols), 0)
    lane8 = lax.broadcasted_iota(jnp.int32, (8, cols), 1)
    row8 = lax.broadcasted_iota(jnp.int32, (8, cols), 0)
    pair = lane >> 1
    even = (lane & 1) == 0
    is_first, is_last = lane == 0, lane == cols - 1
    is_edge = is_first | is_last
    zero = jnp.zeros((rows, cols), jnp.float32)
    blank = jnp.zeros((1, cols), jnp.float32)

    def to_west(x):
        return pltpu.roll(x, cols - 1, 1)

    def to_east(x):
        return pltpu.roll(x, 1, 1)

    def drain(ref, sem):
        pltpu.make_async_copy(ref, ref, sem).wait()

    def send(src, dst, kind, sem, where):
        pltpu.make_async_remote_copy(
            src_ref=src, dst_ref=dst, send_sem=send_sem.at[kind], recv_sem=sem, device_id=where, device_id_type=MESH
        ).start()

    def clear(k, c):
        for m in range(own):
            p[m, k, PAD - 1 : PAD, :] = blank
            p[m, k, PAD + rows : PAD + rows + 1, :] = blank
            v[m, k, rows : rows + 1, :] = blank
        sig[k, PAD - 1 : PAD, :] = blank
        sig[k, PAD + rows : PAD + rows + 1, :] = blank
        return c

    def pack(m):
        def one(k, packed):
            pk = p[m, k, body, :]
            ends = jnp.where(is_last, pk, u[m, k] - horiz_ratio * pk)
            first_row[m, pl.ds(k, 1), :] = v[m, k, 0:1, :] - horiz_ratio * p[m, k, PAD : PAD + 1, :]
            return jnp.where(pair == k, pltpu.roll(ends, 2 * k + 1, 1), packed)

        edge[m] = unrolled(levels, one, zero, 25)

    def pivots():
        def one(i, c):
            k = i + 1
            below, gprev, mass_below, value = c
            sk = s[k]
            hs[k] = horiz_ratio * sk
            vs[k] = vert_ratio * sk
            b = (vert_ratio * vert_ratio) * sk
            mass = thick[k] * sk
            r = 1.0 / (1.0 + b + below - below * gprev)
            gk = b * r
            bi = below * r
            value = (vert_ratio * (mass - mass_below)) * r + bi * value
            inv[k] = r
            binv[k] = bi
            g[k] = gk
            lam[k] = value
            return b, gk, mass, value

        s0 = s[0]
        hs[0] = horiz_ratio * s0
        vs[0] = vert_ratio * s0
        unrolled(levels - 1, one, ((vert_ratio * vert_ratio) * s0, zero, thick[0] * s0, zero))

    def adjoint():
        def weights(k, here, above, packed):
            mk = thick[k] - vert_ratio * (here - above)
            sk = (horiz_ratio * mk) * hs[k]
            mu[k] = mk
            sig[k, body, :] = sk
            sig_east[k] = to_west(sk)
            sig_west[k] = to_east(sk)
            alpha[k] = mk - 4.0 * sk
            return jnp.where(pair == k, pltpu.roll(sk, 2 * k + 1, 1), packed)

        def two(i, c):
            k = levels - 1 - i
            above, packed = c
            here = lam[k] + g[k] * above
            lam[k] = here
            return here, weights(k, here, above, packed)

        above, packed = unrolled(levels - 1, two, (zero, zero), 49)
        sig_edge[...] = weights(0, zero, above, packed)

    def diverge(m):
        def one(k, c):
            usum, vsum, psum = c
            pk, uk, vk = p[m, k, body, :], u[m, k], v[m, k, pl.ds(0, rows), :]
            around = to_east(pk) + (p[m, k, pl.ds(PAD - 1, rows), :] + p[m, k, pl.ds(PAD + 1, rows), :])
            div = (to_west(uk - horiz_ratio * pk) - uk) + (v[m, k, pl.ds(1, rows), :] - vk)
            u[m, k] = div - horiz_ratio * (around - 4.0 * pk)
            tk = thick[k]
            return usum + tk * uk, vsum + tk * vk, psum + tk * pk

        return unrolled(levels, one, (zero, zero, zero), 50)

    def forward(m):
        mine = edge[m]
        halo = jnp.where(
            even, -horiz_ratio * (edge_recv[m, 0] - mine), pltpu.roll(edge_recv[m, 1] - mine, cols - 2, 1))

        def level(k, rest):
            hk = pltpu.roll(halo, cols - 2 * k if not isinstance(k, int) or k > 0 else 0, 1)
            div = u[m, k] + jnp.where(is_edge, hk, 0.0)
            low = jnp.where(row8 == 0, -horiz_ratio * row_recv[m, 0, pl.ds(k, 1), :], 0.0)
            high = jnp.where(row8 == 7, row_recv[m, 1, pl.ds(k, 1), :], 0.0)
            div = jnp.concatenate([div[:8] + low, div[8 : rows - 8], div[rows - 8 :] + high], axis=0)
            e = hs[k] * div
            pa = p[m, k, body, :] - e
            part[m, k] = pa
            return pa, rest - mu[k] * e

        def one(i, c):
            k = i + 1
            pa_below, value, rest = c
            pa, rest = level(k, rest)
            rhs = w[m, i] - vert_ratio * (pa - pa_below)
            value = rhs * inv[k] + binv[k] * value
            w[m, i] = value
            return pa, value, rest

        pa, rest = level(0, zero)
        return unrolled(levels - 1, one, (pa, zero, rest), 49)[2]

    def backward(m, rest):
        def weigh(k, pk, packed, mass, rest, te, tw, tn, ts):
            p_rows[m, 0, pl.ds(k, 1), :] = pk[0:1]
            p_rows[m, 1, pl.ds(k, 1), :] = pk[rows - 1 : rows]
            return (
                jnp.where(pair == k, pltpu.roll(pk, 2 * k + 1, 1), packed),
                mass + thick[k] * pk,
                rest + alpha[k] * pk,
                te + sig_east[k] * pk,
                tw + sig_west[k] * pk,
                tn + sig[k, pl.ds(PAD + 1, rows), :] * pk,
                ts + sig[k, pl.ds(PAD - 1, rows), :] * pk,
            )

        def one(i, c):
            k = levels - 1 - i
            above, packed, mass, rest, *sides = c
            here = w[m, k - 1] + g[k] * above
            pk = part[m, k] - vs[k] * (above - here)
            return (here, *weigh(k, pk, packed, mass, rest + lam[k] * here, *sides))

        above, *sums = unrolled(levels - 1, one, (zero, zero, zero, rest, zero, zero, zero, zero), 49)
        packed, *sums = weigh(0, part[m, 0] - vs[0] * above, *sums)
        p_edge[m] = packed
        return sums

    def whole(m, usum, vsum, q, rest, te, tw, tn, ts):
        total = rest + jnp.where(is_first, 0.0, to_east(te)) + jnp.where(is_last, 0.0, to_west(tw))
        total = total + pltpu.roll(tn, 1, 0) + pltpu.roll(ts, rows - 1, 0)
        ue = usum - horiz_ratio * (q - jnp.where(is_first, 0.0, to_east(q)))
        vn = vsum - horiz_ratio * (q - jnp.where(row == 0, 0.0, pltpu.roll(q, 1, 0)))
        for r in range(n_mem):
            for f, x in enumerate((total, ue, vn)):
                integ[m, r, f] = x[r * quarter : (r + 1) * quarter]
        for i in range(1, n_mem):
            other = lax.rem(mem + i, n_mem)
            send(integ.at[m, other], gath.at[mem, m], 4, recv_sem.at[2], {"mem": other})

    def rims(qs):
        sig_e, sig_w = pltpu.roll(sig_edge_recv[1], cols - 1, 1), pltpu.roll(sig_edge_recv[0], 1, 1)
        rims = zero
        for m in range(own):
            te = jnp.sum(jnp.where(even, sig_e * p_edge[m], 0.0), axis=1, keepdims=True)
            tw = jnp.sum(jnp.where(even, 0.0, sig_w * p_edge[m]), axis=1, keepdims=True)
            rims = jnp.where(lane == 2 * m, te, rims)
            rims = jnp.where(lane == 2 * m + 1, pltpu.roll(qs[m], 2 * m + 2, 1), rims)
            rims = jnp.where(lane == cols - 1 - m, tw, rims)
        for r in range(n_mem):
            rim[r] = rims[r * quarter : (r + 1) * quarter]
        for i in range(n_mem):
            other = lax.rem(mem + i, n_mem)
            send(rim.at[other], rim_recv.at[0, mem], 5, recv_sem.at[3], {"mem": other, "tx": east})
            send(rim.at[other], rim_recv.at[1, mem], 5, recv_sem.at[3], {"mem": other, "tx": west})

    def lips(qs):
        for m in range(own):
            lip[m : m + 1, :] = jnp.sum(sig_rows[0] * p_rows[m, 1], axis=0, keepdims=True)
            lip[own + m : own + m + 1, :] = qs[m][rows - 1 : rows]
            lip[2 * own + m : 2 * own + m + 1, :] = jnp.sum(sig_rows[1] * p_rows[m, 0], axis=0, keepdims=True)
        send(lip, lip_recv.at[0, mem], 6, recv_sem.at[4], {"mem": 0, "ty": north})
        send(lip, lip_recv.at[1, mem], 6, recv_sem.at[4], {"mem": n_mem - 1, "ty": south})

    with scope("clear"):
        unrolled(levels, clear, 0, 10)
    with scope("wait_s"):
        loads["s"].wait()
        for copy in small:
            copy.wait()
    with scope("pivots"):
        pivots()
    for m in range(own):
        with scope(f"wait_load{m}"):
            for name in "puv":
                loads[name, m].wait()
        with scope(f"pack{m}"):
            pack(m)
        if m == 0:
            with scope("wait_barrier"):
                pl.semaphore_wait(barrier, len(greet))
        with scope("send"):
            send(p.at[m, :, PAD + rows - 1, :], row_recv.at[m, 0], 0, member_sem.at[m, 0], {"ty": north})
            send(first_row.at[m], row_recv.at[m, 1], 0, member_sem.at[m, 0], {"ty": south})
            send(edge.at[m], edge_recv.at[m, 0], 1, member_sem.at[m, 1], {"tx": east})
            send(edge.at[m], edge_recv.at[m, 1], 1, member_sem.at[m, 1], {"tx": west})
    with scope("adjoint"):
        adjoint()
    with scope("send_sig"):
        send(sig_edge, sig_edge_recv.at[0], 2, recv_sem.at[0], {"tx": east})
        send(sig_edge, sig_edge_recv.at[1], 2, recv_sem.at[0], {"tx": west})
        send(sig.at[:, PAD, :], sig_rows.at[0], 3, recv_sem.at[1], {"ty": south})
        send(sig.at[:, PAD + rows - 1, :], sig_rows.at[1], 3, recv_sem.at[1], {"ty": north})
    sums = []
    for m in range(own):
        with scope(f"diverge{m}"):
            sums.append(diverge(m))

    qs = []
    for m in range(own):
        with scope(f"wait_edge{m}"):
            if m == 0:
                loads["w"].wait()
            drain(edge_recv.at[m], member_sem.at[m, 1])
        with scope(f"wait_row{m}"):
            drain(row_recv.at[m], member_sem.at[m, 0])
        with scope(f"forward{m}"):
            rest = forward(m)
        with scope(f"backward{m}"):
            mass, *rest = backward(m, rest)
        qs.append(sums[m][2] + mass)
        if m == own - 1:
            with scope("wait_sig"):
                drain(sig_edge_recv, recv_sem.at[0])
            with scope("rims"):
                rims(qs)
        with scope(f"whole{m}"):
            whole(m, sums[m][0], sums[m][1], qs[m], *rest)
    with scope("wait_sig_rows"):
        drain(sig_rows, recv_sem.at[1])
    with scope("lips"):
        lips(qs)

    bottom = (row8[:quarter] == 0) & (mem == 0)
    top = (row8[:quarter] == quarter - 1) & (mem == n_mem - 1)
    with scope("wait_lip"):

        @pl.when((mem == 0) | (mem == n_mem - 1))
        def _():
            drain(lip_recv.at[0], recv_sem.at[4])

    with scope("wait_rim"):
        drain(rim_recv, recv_sem.at[3])
    with scope("wait_mem"):
        drain(gath.at[pl.ds(0, n_mem - 1)], recv_sem.at[2])

    with scope("stats"):
        fields = []
        lane_q = lane[:quarter]
        for i in range(n_mem):
            other = lax.rem(mem + i, n_mem)
            from_west, from_east = rim_recv[0, other], rim_recv[1, other]
            from_south, from_north = lip_recv[0, other], lip_recv[1, other]
            for m in range(own):
                source = integ.at[m, mem] if i == 0 else gath.at[other, m]
                total, ue, vn = (source[f] for f in range(3))
                te = from_west if m == 0 else pltpu.roll(from_west, cols - 2 * m, 1)
                tw = from_east if m == 0 else pltpu.roll(from_east, m, 1)
                total = total + jnp.where(lane_q == 0, te, 0.0) + jnp.where(lane_q == cols - 1, tw, 0.0)
                total = total + jnp.where(bottom, from_south[m : m + 1], 0.0)
                total = total + jnp.where(top, from_north[2 * own + m : 2 * own + m + 1], 0.0)
                ue = ue + horiz_ratio * jnp.where(lane_q == 0, pltpu.roll(from_west, cols - 2 * m - 1, 1), 0.0)
                vn = vn + horiz_ratio * jnp.where(bottom, from_south[own + m : own + m + 1], 0.0)
                fields.append([total, ue, vn])

        members = len(fields)
        for f in range(3):
            total = fields[0][f]
            for one in fields[1:]:
                total = total + one[f]
            mean = total / members
            second = (fields[0][f] - mean) ** 2
            for one in fields[1:]:
                second = second + (one[f] - mean) ** 2
            everyone[me, f] = mean
            everyone[me, 3 + f] = second / (members - 1)

        far = lambda d: -(min(d[0], n_ty - d[0]) + min(d[1], n_tx - d[1]))
        offsets = sorted([(a, b) for a in range(n_ty) for b in range(n_tx)], key=far)[:-1]
        for a, b in offsets:
            where = {"ty": lax.rem(ty + a, n_ty), "tx": lax.rem(tx + b, n_tx)}
            send(everyone.at[me], everyone.at[me], 7, recv_sem.at[5], where)
    mine = jnp.int32(0)
    for t in range(tiles):
        mine = jnp.where(owner[t] == me, t, mine)
    with scope("wait_all"):
        drain(everyone.at[pl.ds(0, tiles - 1)], recv_sem.at[5])
    with scope("finish"):
        out[0, 0] = everyone[mine]
        drain(row_recv, send_sem.at[0])
        drain(edge_recv, send_sem.at[1])
        drain(sig_edge_recv, send_sem.at[2])
        drain(sig_rows, send_sem.at[3])
        drain(gath.at[pl.ds(0, n_mem - 1)], send_sem.at[4])
        drain(rim_recv, send_sem.at[5])
        drain(lip_recv.at[0, pl.ds(0, 2)], send_sem.at[6])
        drain(everyone.at[pl.ds(0, tiles - 1)], send_sem.at[7])


def solution(mesh):
    n_mem, n_ty, n_tx = (mesh.shape[a] for a in ("mem", "ty", "tx"))
    tiles = n_ty * n_tx

    def local(pressure, east_wind, north_wind, vertical_wind, sound_squared, thickness, owner_map):
        own, levels, rows, cols = pressure.shape
        quarter = rows // n_mem
        f32 = jnp.float32
        dma = pltpu.SemaphoreType.DMA

        def vmem(*shape):
            return pltpu.VMEM(shape, f32)

        return pl.pallas_call(
            functools.partial(kernel, (n_mem, n_ty, n_tx)),
            name="acoustic",
            out_shape=pltpu.VMEM((1, 1, 6, quarter, cols), f32),
            in_specs=[pl.BlockSpec(memory_space=pl.ANY)] * 7,
            out_specs=pl.BlockSpec(memory_space=pltpu.VMEM),
            scratch_shapes=[
                vmem(own, levels, rows + 2 * PAD, cols),
                vmem(own, levels, rows, cols),
                vmem(own, levels, rows + PAD, cols),
                vmem(own, levels - 1, rows, cols),
                vmem(levels, rows, cols),
                vmem(own, levels, rows, cols),
                *[vmem(levels, rows, cols)] * 8,
                vmem(levels, rows + 2 * PAD, cols),
                *[vmem(levels, rows, cols)] * 2,
                vmem(own, rows, cols),
                vmem(own, 2, rows, cols),
                vmem(own, levels, cols),
                vmem(own, 2, levels, cols),
                vmem(rows, cols),
                vmem(2, rows, cols),
                vmem(2, levels, cols),
                vmem(own, rows, cols),
                vmem(own, 2, levels, cols),
                vmem(own, n_mem, 3, quarter, cols),
                vmem(n_mem, own, 3, quarter, cols),
                vmem(n_mem, quarter, cols),
                vmem(2, n_mem, quarter, cols),
                vmem(-(-3 * own // 8) * 8, cols),
                vmem(2, n_mem, -(-3 * own // 8) * 8, cols),
                vmem(tiles, 6, quarter, cols),
                pltpu.SMEM(thickness.shape, f32),
                pltpu.SMEM(owner_map.shape, jnp.int32),
                dma((3 * own + 2,)),
                dma((2,)),
                dma((8,)),
                dma((own, 2)),
                dma((6,)),
            ],
            compiler_params=pltpu.CompilerParams(collective_id=0, has_side_effects=True),
        )(pressure, east_wind, north_wind, vertical_wind, sound_squared, thickness, owner_map)

    field = P("mem", None, "ty", "tx")
    return jax.shard_map(
        local,
        mesh=mesh,
        in_specs=(field, field, field, field, P(None, "ty", "tx"), P(), P()),
        out_specs=P("ty", "tx", None, "mem", None),
        check_vma=False,
    )
```

```python
import functools

import jax
import jax.numpy as jnp
from jax import lax
from jax.experimental import pallas as pl
from jax.experimental.pallas import tpu as pltpu
from jax.sharding import PartitionSpec as P

MESH = pl.DeviceIdType.MESH
PAD = 8

horiz_ratio = 0.35
vert_ratio = 1.5


def unrolled(count, body, carry, most=7):
    trips = -(-count // most)
    width = count // trips
    first = count - trips * width

    def block(i, c):
        for j in range(width):
            c = body(first + i * width + j, c)
        return c

    for i in range(first):
        carry = body(i, carry)
    return lax.fori_loop(0, trips, block, carry)


def layout(n_ty, n_tx):
    homes = sorted({(0, 0), (n_ty // 2, n_tx // 2)})

    def far(o, h):
        a, b = (o[0] - h[0]) % n_ty, (o[1] - h[1]) % n_tx
        return min(a, n_ty - a) + min(b, n_tx - b)

    serve, hops = {}, set()
    for o in ((a, b) for a in range(n_ty) for b in range(n_tx)):
        n = min(range(len(homes)), key=lambda i: far(o, homes[i]))
        serve[o] = n
        hops.add(((o[0] - homes[n][0]) % n_ty, (o[1] - homes[n][1]) % n_tx))
    return homes, serve, sorted(hops - {(0, 0)}, key=lambda d: (-far(d, (0, 0)), d))


def kernel(
    sizes,
    p_hbm, u_hbm, v_hbm, w_hbm, s_hbm, thick_hbm, owner_hbm,
    out,
    p, u, v, w, s, part, hs, vs, inv, binv, g, lam, mu, alpha, sig, sig_east, sig_west,
    edge, edge_recv, first_row, row_recv, sig_edge, sig_edge_recv, sig_rows, p_edge, p_rows,
    integ, gath, rim, rim_recv, lip, lip_recv, held, chosen, arrived, thick, owner,
    load_sem, small_sem, send_sem, member_sem, recv_sem, round_sem,
):
    n_mem, n_ty, n_tx = sizes
    own, levels, rows, cols = u.shape
    quarter = rows // n_mem
    body = pl.ds(PAD, rows)
    mem, ty, tx = lax.axis_index("mem"), lax.axis_index("ty"), lax.axis_index("tx")
    me = ty * n_tx + tx
    east, west = lax.rem(tx + 1, n_tx), lax.rem(tx + n_tx - 1, n_tx)
    north, south = lax.rem(ty + 1, n_ty), lax.rem(ty + n_ty - 1, n_ty)
    scope = jax.named_scope

    homes, serve, hops = layout(n_ty, n_tx)
    sides = [(0, 1), (0, n_tx - 1), (1, 0), (n_ty - 1, 0)]

    def shift(*offsets):
        return sum(o[0] for o in offsets) % n_ty, sum(o[1] for o in offsets) % n_tx

    def place(*offsets, **at):
        a, b = shift(*offsets)
        return {"ty": lax.rem(ty + a, n_ty), "tx": lax.rem(tx + b, n_tx), **at}

    def member(i):
        return {"mem": lax.rem(mem + i, n_mem)}

    across, along = [place(o) for o in sides[:2]], [place(o) for o in sides[2:]]
    others = [member(i) for i in range(1, n_mem)]
    rounds = [across] * (n_tx // 2 - 1) + [along] * (n_ty // 2) + [others]

    def greet(sem, peers):
        for where in peers:
            pl.semaphore_signal(sem, inc=1, device_id=where, device_id_type=MESH)

    near = across + along + others
    barrier = pltpu.get_barrier_semaphore()
    greet(barrier, near)
    met = []

    def meet(more):
        for _ in range(more):
            n = len(met)
            if n == 0:
                pl.semaphore_wait(barrier, len(near))
            elif n <= len(rounds):
                pl.semaphore_wait(round_sem.at[n - 1], len(rounds[n - 1]))
            if n < len(rounds):
                greet(round_sem.at[n], rounds[n])
            met.append(n)

    def load(src, dst, sem):
        copy = pltpu.make_async_copy(src, dst, sem)
        copy.start()
        return copy

    loads = {}
    for m in range(own):
        loads["p", m] = load(p_hbm.at[m], p.at[m, :, body, :], load_sem.at[3 * m])
        loads["v", m] = load(v_hbm.at[m], v.at[m, :, pl.ds(0, rows), :], load_sem.at[3 * m + 1])
        loads["u", m] = load(u_hbm.at[m], u.at[m], load_sem.at[3 * m + 2])
        if m == 0:
            small = [load(thick_hbm, thick, small_sem.at[0]), load(owner_hbm, owner, small_sem.at[1])]
            loads["s"] = load(s_hbm, s, load_sem.at[3 * own])
    loads["w"] = load(w_hbm, w, load_sem.at[3 * own + 1])

    lane = lax.broadcasted_iota(jnp.int32, (rows, cols), 1)
    row = lax.broadcasted_iota(jnp.int32, (rows, cols), 0)
    lane8 = lax.broadcasted_iota(jnp.int32, (8, cols), 1)
    row8 = lax.broadcasted_iota(jnp.int32, (8, cols), 0)
    pair = lane >> 1
    even = (lane & 1) == 0
    is_first, is_last = lane == 0, lane == cols - 1
    is_edge = is_first | is_last
    zero = jnp.zeros((rows, cols), jnp.float32)
    blank = jnp.zeros((1, cols), jnp.float32)

    def to_west(x):
        return pltpu.roll(x, cols - 1, 1)

    def to_east(x):
        return pltpu.roll(x, 1, 1)

    def drain(ref, sem):
        pltpu.make_async_copy(ref, ref, sem).wait()

    def send(src, dst, kind, sem, where):
        pltpu.make_async_remote_copy(
            src_ref=src, dst_ref=dst, send_sem=send_sem.at[kind], recv_sem=sem, device_id=where, device_id_type=MESH
        ).start()

    def clear(k, c):
        for m in range(own):
            p[m, k, PAD - 1 : PAD, :] = blank
            p[m, k, PAD + rows : PAD + rows + 1, :] = blank
            v[m, k, rows : rows + 1, :] = blank
        sig[k, PAD - 1 : PAD, :] = blank
        sig[k, PAD + rows : PAD + rows + 1, :] = blank
        return c

    def pack(m):
        def one(k, packed):
            pk = p[m, k, body, :]
            ends = jnp.where(is_last, pk, u[m, k] - horiz_ratio * pk)
            return jnp.where(pair == k, pltpu.roll(ends, 2 * k + 1, 1), packed)

        edge[m] = unrolled(levels, one, zero, 50)

    def pack_rows(m):
        def one(k, c):
            first_row[m, pl.ds(k, 1), :] = v[m, k, 0:1, :] - horiz_ratio * p[m, k, PAD : PAD + 1, :]
            return c

        unrolled(levels, one, 0, 50)

    def pivots():
        def one(i, c):
            k = i + 1
            below, gprev, mass_below, value = c
            sk = s[k]
            hs[k] = horiz_ratio * sk
            vs[k] = vert_ratio * sk
            b = (vert_ratio * vert_ratio) * sk
            mass = thick[k] * sk
            r = 1.0 / (1.0 + b + below - below * gprev)
            gk = b * r
            bi = below * r
            value = (vert_ratio * (mass - mass_below)) * r + bi * value
            inv[k] = r
            binv[k] = bi
            g[k] = gk
            lam[k] = value
            return b, gk, mass, value

        s0 = s[0]
        hs[0] = horiz_ratio * s0
        vs[0] = vert_ratio * s0
        unrolled(levels - 1, one, ((vert_ratio * vert_ratio) * s0, zero, thick[0] * s0, zero))

    def adjoint():
        def weights(k, here, above, packed):
            mk = thick[k] - vert_ratio * (here - above)
            sk = (horiz_ratio * mk) * hs[k]
            mu[k] = mk
            sig[k, body, :] = sk
            sig_east[k] = to_west(sk)
            sig_west[k] = to_east(sk)
            alpha[k] = mk - 4.0 * sk
            return jnp.where(pair == k, pltpu.roll(sk, 2 * k + 1, 1), packed)

        def two(i, c):
            k = levels - 1 - i
            above, packed = c
            here = lam[k] + g[k] * above
            lam[k] = here
            return here, weights(k, here, above, packed)

        above, packed = unrolled(levels - 1, two, (zero, zero), 49)
        sig_edge[...] = weights(0, zero, above, packed)

    def diverge(m):
        def one(k, c):
            usum, vsum, psum = c
            pk, uk, vk = p[m, k, body, :], u[m, k], v[m, k, pl.ds(0, rows), :]
            around = to_east(pk) + (p[m, k, pl.ds(PAD - 1, rows), :] + p[m, k, pl.ds(PAD + 1, rows), :])
            div = (to_west(uk - horiz_ratio * pk) - uk) + (v[m, k, pl.ds(1, rows), :] - vk)
            u[m, k] = div - horiz_ratio * (around - 4.0 * pk)
            tk = thick[k]
            return usum + tk * uk, vsum + tk * vk, psum + tk * pk

        return unrolled(levels, one, (zero, zero, zero), 50)

    def forward(m):
        mine = edge[m]
        halo = jnp.where(
            even, -horiz_ratio * (edge_recv[m, 0] - mine), pltpu.roll(edge_recv[m, 1] - mine, cols - 2, 1))

        def level(k, rest):
            hk = pltpu.roll(halo, cols - 2 * k if not isinstance(k, int) or k > 0 else 0, 1)
            div = u[m, k] + jnp.where(is_edge, hk, 0.0)
            low = jnp.where(row8 == 0, -horiz_ratio * row_recv[m, 0, pl.ds(k, 1), :], 0.0)
            high = jnp.where(row8 == 7, row_recv[m, 1, pl.ds(k, 1), :], 0.0)
            div = jnp.concatenate([div[:8] + low, div[8 : rows - 8], div[rows - 8 :] + high], axis=0)
            e = hs[k] * div
            pa = p[m, k, body, :] - e
            part[m, k] = pa
            return pa, rest - mu[k] * e

        def one(i, c):
            k = i + 1
            pa_below, value, rest = c
            pa, rest = level(k, rest)
            rhs = w[m, i] - vert_ratio * (pa - pa_below)
            value = rhs * inv[k] + binv[k] * value
            w[m, i] = value
            return pa, value, rest

        pa, rest = level(0, zero)
        return unrolled(levels - 1, one, (pa, zero, rest), 49)[2]

    def backward(m, rest):
        def weigh(k, pk, packed, mass, rest, te, tw, tn, ts):
            p_rows[m, 0, pl.ds(k, 1), :] = pk[0:1]
            p_rows[m, 1, pl.ds(k, 1), :] = pk[rows - 1 : rows]
            return (
                jnp.where(pair == k, pltpu.roll(pk, 2 * k + 1, 1), packed),
                mass + thick[k] * pk,
                rest + alpha[k] * pk,
                te + sig_east[k] * pk,
                tw + sig_west[k] * pk,
                tn + sig[k, pl.ds(PAD + 1, rows), :] * pk,
                ts + sig[k, pl.ds(PAD - 1, rows), :] * pk,
            )

        def one(i, c):
            k = levels - 1 - i
            above, packed, mass, rest, *sides = c
            here = w[m, k - 1] + g[k] * above
            pk = part[m, k] - vs[k] * (above - here)
            return (here, *weigh(k, pk, packed, mass, rest + lam[k] * here, *sides))

        above, *sums = unrolled(levels - 1, one, (zero, zero, zero, rest, zero, zero, zero, zero), 49)
        packed, *sums = weigh(0, part[m, 0] - vs[0] * above, *sums)
        p_edge[m] = packed
        return sums

    def whole(m, usum, vsum, q, rest, te, tw, tn, ts):
        total = rest + jnp.where(is_first, 0.0, to_east(te)) + jnp.where(is_last, 0.0, to_west(tw))
        total = total + pltpu.roll(tn, 1, 0) + pltpu.roll(ts, rows - 1, 0)
        ue = usum - horiz_ratio * (q - jnp.where(is_first, 0.0, to_east(q)))
        vn = vsum - horiz_ratio * (q - jnp.where(row == 0, 0.0, pltpu.roll(q, 1, 0)))
        for r in range(n_mem):
            for f, x in enumerate((total, ue, vn)):
                integ[m, r, f] = x[r * quarter : (r + 1) * quarter]

    def send_whole(m):
        for n, h in reversed(list(enumerate(homes))):
            for i in range(0 if n else 1, n_mem):
                other = lax.rem(mem + i, n_mem)
                send(integ.at[m, other], gath.at[n * n_mem + mem, m], 4, recv_sem.at[2], place(h, mem=other))

    def rims(qs):
        sig_e, sig_w = pltpu.roll(sig_edge_recv[1], cols - 1, 1), pltpu.roll(sig_edge_recv[0], 1, 1)
        rims = zero
        for m in range(own):
            te = jnp.sum(jnp.where(even, sig_e * p_edge[m], 0.0), axis=1, keepdims=True)
            tw = jnp.sum(jnp.where(even, 0.0, sig_w * p_edge[m]), axis=1, keepdims=True)
            rims = jnp.where(lane == 2 * m, te, rims)
            rims = jnp.where(lane == 2 * m + 1, pltpu.roll(qs[m], 2 * m + 2, 1), rims)
            rims = jnp.where(lane == 2 * own + m, tw, rims)
        rims = jnp.where(lane < 4 * own, rims, 0.0)
        for r in range(n_mem):
            piece = rims[r * quarter : (r + 1) * quarter]
            piece = pltpu.roll(piece, 0, 1, stride=8, stride_axis=0)
            rim[r] = jnp.sum(piece, axis=0, keepdims=True)

    def send_rims():
        for n, h in reversed(list(enumerate(homes))):
            for i in range(n_mem):
                other = lax.rem(mem + i, n_mem)
                for kind in range(2):
                    send(
                        rim.at[other], rim_recv.at[n, kind, mem], 5, recv_sem.at[3],
                        place(h, sides[kind], mem=other))

    def lips(qs):
        for m in range(own):
            lip[m : m + 1, :] = jnp.sum(sig_rows[0] * p_rows[m, 1], axis=0, keepdims=True)
            lip[own + m : own + m + 1, :] = qs[m][rows - 1 : rows]
            lip[2 * own + m : 2 * own + m + 1, :] = jnp.sum(sig_rows[1] * p_rows[m, 0], axis=0, keepdims=True)

    def send_lips():
        for n, h in reversed(list(enumerate(homes))):
            for kind, goal in enumerate((0, n_mem - 1)):
                send(lip, lip_recv.at[kind, n, mem], 6, recv_sem.at[4], place(h, sides[2 + kind], mem=goal))

    with scope("clear"):
        unrolled(levels, clear, 0, 10)
    for m in range(own):
        with scope(f"wait_pv{m}"):
            loads["p", m].wait()
            loads["v", m].wait()
        with scope(f"rows{m}"):
            pack_rows(m)
        if m == 0:
            with scope("wait_barrier"):
                meet(1)
        with scope(f"send_rows{m}"):
            send(p.at[m, :, PAD + rows - 1, :], row_recv.at[m, 0], 0, member_sem.at[m, 0], {"ty": north})
            send(first_row.at[m], row_recv.at[m, 1], 0, member_sem.at[m, 0], {"ty": south})
        with scope(f"wait_u{m}"):
            loads["u", m].wait()
        with scope(f"pack{m}"):
            pack(m)
            send(edge.at[m], edge_recv.at[m, 0], 1, member_sem.at[m, 1], {"tx": east})
            send(edge.at[m], edge_recv.at[m, 1], 1, member_sem.at[m, 1], {"tx": west})
        if m == 0:
            with scope("wait_s"):
                loads["s"].wait()
                for copy in small:
                    copy.wait()
            with scope("pivots"):
                pivots()
    with scope("adjoint"):
        adjoint()
    with scope("send_sig"):
        send(sig_edge, sig_edge_recv.at[0], 2, recv_sem.at[0], {"tx": east})
        send(sig_edge, sig_edge_recv.at[1], 2, recv_sem.at[0], {"tx": west})
        send(sig.at[:, PAD, :], sig_rows.at[0], 3, recv_sem.at[1], {"ty": south})
        send(sig.at[:, PAD + rows - 1, :], sig_rows.at[1], 3, recv_sem.at[1], {"ty": north})
    sums = []
    for m in range(own):
        with scope(f"diverge{m}"):
            sums.append(diverge(m))

    qs = []
    with scope("meet0"):
        meet(1)
    for m in range(own):
        with scope(f"wait_edge{m}"):
            if m == 0:
                loads["w"].wait()
            drain(edge_recv.at[m], member_sem.at[m, 1])
        with scope(f"wait_row{m}"):
            drain(row_recv.at[m], member_sem.at[m, 0])
        with scope(f"forward{m}"):
            rest = forward(m)
        with scope(f"meet{m + 1}"):
            if m == 0:
                meet(1)
            else:
                meet(len(rounds) + 1 - len(met))
                send_whole(m - 1)
        with scope(f"backward{m}"):
            mass, *rest = backward(m, rest)
        qs.append(sums[m][2] + mass)
        last = m == own - 1
        if last:
            with scope("wait_sig"):
                meet(len(rounds) + 1 - len(met))
                drain(sig_edge_recv, recv_sem.at[0])
                drain(sig_rows, recv_sem.at[1])
        with scope(f"sums{m}"):
            if last:
                rims(qs)
                lips(qs)
            whole(m, sums[m][0], sums[m][1], qs[m], *rest)
        with scope(f"send_sums{m}"):
            if last:
                send_rims()
                send_lips()
                send_whole(m)

    bottom = (row8[:quarter] == 0) & (mem == 0)
    top = (row8[:quarter] == quarter - 1) & (mem == n_mem - 1)
    with scope("wait_lip"):

        @pl.when((mem == 0) | (mem == n_mem - 1))
        def _():
            drain(lip_recv.at[0], recv_sem.at[4])

    with scope("wait_rim"):
        drain(rim_recv, recv_sem.at[3])
    with scope("wait_mem"):
        drain(gath.at[pl.ds(0, len(homes) * n_mem - 1)], recv_sem.at[2])

    lane_q = lane[:quarter]

    column_of = lane_q - 8 * row[:quarter]

    def column(x, c):
        return jnp.sum(jnp.where(column_of == c, x, 0.0), axis=1, keepdims=True)

    def stats(n):
        fields = []
        for i in range(n_mem):
            other = lax.rem(mem + i, n_mem)
            from_west, from_east = rim_recv[n, 0, other], rim_recv[n, 1, other]
            from_south, from_north = lip_recv[0, n, other], lip_recv[1, n, other]
            for m in range(own):
                source = integ.at[m, mem] if n == 0 and i == 0 else gath.at[n * n_mem + other, m]
                total, ue, vn = (source[f] for f in range(3))
                te, qw = column(from_west, 2 * m), column(from_west, 2 * m + 1)
                tw = column(from_east, 2 * own + m)
                total = total + jnp.where(lane_q == 0, te, 0.0) + jnp.where(lane_q == cols - 1, tw, 0.0)
                total = total + jnp.where(bottom, from_south[m : m + 1], 0.0)
                total = total + jnp.where(top, from_north[2 * own + m : 2 * own + m + 1], 0.0)
                ue = ue + horiz_ratio * jnp.where(lane_q == 0, qw, 0.0)
                vn = vn + horiz_ratio * jnp.where(bottom, from_south[own + m : own + m + 1], 0.0)
                fields.append([total, ue, vn])

        members = len(fields)
        for f in range(3):
            total = fields[0][f]
            for one in fields[1:]:
                total = total + one[f]
            mean = total / members
            second = (fields[0][f] - mean) ** 2
            for one in fields[1:]:
                second = second + (one[f] - mean) ** 2
            held[n, f] = mean
            held[n, 3 + f] = second / (members - 1)

    def number(o):
        where = place(o)
        return where["ty"] * n_tx + where["tx"]

    def back(o):
        return (-o[0] % n_ty, -o[1] % n_tx)

    with scope("stats"):
        for n in range(len(homes)):
            stats(n)
        for i, hop in enumerate(hops):
            pick = jnp.int32(0)
            for n, h in enumerate(homes):
                if serve[shift(hop, h)] == n:
                    pick = jnp.where(owner[number(back(h))] == number(hop), n, pick)
            chosen[i] = held[pick]
            send(chosen.at[i], arrived.at[i], 7, recv_sem.at[5], place(hop))
        here, there, local = jnp.int32(0), jnp.int32(0), jnp.int32(0)
        for o, n in serve.items():
            found = owner[number(back(o))] == me
            hop = shift(o, back(homes[n]))
            if hop == (0, 0):
                here = jnp.where(found, n, here)
                local = jnp.where(found, 1, local)
            else:
                there = jnp.where(found, hops.index(hop), there)
    with scope("wait_all"):
        drain(arrived, recv_sem.at[5])
    with scope("finish"):
        out[0, 0] = jnp.where(local == 1, held[here], arrived[there])
        drain(row_recv, send_sem.at[0])
        drain(edge_recv, send_sem.at[1])
        drain(sig_edge_recv, send_sem.at[2])
        drain(sig_rows, send_sem.at[3])
        drain(gath.at[pl.ds(0, len(homes) * n_mem - 1)], send_sem.at[4])
        drain(rim_recv, send_sem.at[5])
        drain(lip_recv.at[0, :, pl.ds(0, 2)], send_sem.at[6])
        drain(arrived, send_sem.at[7])


def solution(mesh):
    n_mem, n_ty, n_tx = (mesh.shape[a] for a in ("mem", "ty", "tx"))
    homes, _, hops = layout(n_ty, n_tx)
    rounds = n_tx // 2 + n_ty // 2

    def local(pressure, east_wind, north_wind, vertical_wind, sound_squared, thickness, owner_map):
        own, levels, rows, cols = pressure.shape
        quarter = rows // n_mem
        f32 = jnp.float32
        dma = pltpu.SemaphoreType.DMA

        def vmem(*shape):
            return pltpu.VMEM(shape, f32)

        return pl.pallas_call(
            functools.partial(kernel, (n_mem, n_ty, n_tx)),
            name="acoustic",
            out_shape=pltpu.VMEM((1, 1, 6, quarter, cols), f32),
            in_specs=[pl.BlockSpec(memory_space=pl.ANY)] * 7,
            out_specs=pl.BlockSpec(memory_space=pltpu.VMEM),
            scratch_shapes=[
                vmem(own, levels, rows + 2 * PAD, cols),
                vmem(own, levels, rows, cols),
                vmem(own, levels, rows + PAD, cols),
                vmem(own, levels - 1, rows, cols),
                vmem(levels, rows, cols),
                vmem(own, levels, rows, cols),
                *[vmem(levels, rows, cols)] * 8,
                vmem(levels, rows + 2 * PAD, cols),
                *[vmem(levels, rows, cols)] * 2,
                vmem(own, rows, cols),
                vmem(own, 2, rows, cols),
                vmem(own, levels, cols),
                vmem(own, 2, levels, cols),
                vmem(rows, cols),
                vmem(2, rows, cols),
                vmem(2, levels, cols),
                vmem(own, rows, cols),
                vmem(own, 2, levels, cols),
                vmem(own, n_mem, 3, quarter, cols),
                vmem(len(homes) * n_mem, own, 3, quarter, cols),
                vmem(n_mem, 1, cols),
                vmem(len(homes), 2, n_mem, 1, cols),
                vmem(-(-3 * own // 8) * 8, cols),
                vmem(2, len(homes), n_mem, -(-3 * own // 8) * 8, cols),
                vmem(len(homes), 6, quarter, cols),
                vmem(len(hops), 6, quarter, cols),
                vmem(len(hops), 6, quarter, cols),
                pltpu.SMEM(thickness.shape, f32),
                pltpu.SMEM(owner_map.shape, jnp.int32),
                dma((3 * own + 2,)),
                dma((2,)),
                dma((8,)),
                dma((own, 2)),
                dma((6,)),
                pltpu.SemaphoreType.REGULAR((rounds,)),
            ],
            compiler_params=pltpu.CompilerParams(collective_id=0, has_side_effects=True),
        )(pressure, east_wind, north_wind, vertical_wind, sound_squared, thickness, owner_map)

    field = P("mem", None, "ty", "tx")
    return jax.shard_map(
        local,
        mesh=mesh,
        in_specs=(field, field, field, field, P(None, "ty", "tx"), P(), P()),
        out_specs=P("ty", "tx", None, "mem", None),
        check_vma=False,
    )
```

```python
import functools

import jax
import jax.numpy as jnp
from jax import lax
from jax.experimental import pallas as pl
from jax.experimental.pallas import tpu as pltpu
from jax.sharding import PartitionSpec as P

MESH = pl.DeviceIdType.MESH
PAD = 8

horiz_ratio = 0.35
vert_ratio = 1.5


def unrolled(count, body, carry, most=7):
    trips = -(-count // most)
    width = count // trips
    first = count - trips * width

    def block(i, c):
        for j in range(width):
            c = body(first + i * width + j, c)
        return c

    for i in range(first):
        carry = body(i, carry)
    return lax.fori_loop(0, trips, block, carry)


def layout(n_ty, n_tx):
    homes = sorted({(0, 0), (n_ty // 2, 0)})

    def far(o, h):
        a, b = (o[0] - h[0]) % n_ty, (o[1] - h[1]) % n_tx
        return min(a, n_ty - a) + min(b, n_tx - b)

    serve, hops = {}, set()
    for o in ((a, b) for a in range(n_ty) for b in range(n_tx)):
        n = min(range(len(homes)), key=lambda i: far(o, homes[i]))
        serve[o] = n
        hops.add(((o[0] - homes[n][0]) % n_ty, (o[1] - homes[n][1]) % n_tx))
    sides = [(0, 1), (0, n_tx - 1), (1, 0), (n_ty - 1, 0)]
    reach = max(far(((a + c) % n_ty, (b + d) % n_tx), (0, 0)) for a, b in homes for c, d in sides + [(0, 0)])
    reach = max(reach, *(far(d, (0, 0)) for d in hops))
    return homes, serve, sorted(hops - {(0, 0)}, key=lambda d: (-far(d, (0, 0)), d)), sides, reach


def kernel(
    sizes,
    p_hbm, u_hbm, v_hbm, w_hbm, s_hbm, thick_hbm, owner_hbm,
    out,
    p, u, v, w, s, part, hs, vs, inv, binv, g, lam, mu, alpha, sig, sig_east, sig_west,
    edge, edge_recv, first_row, row_recv, sig_edge, sig_edge_recv, sig_rows, p_edge, p_rows,
    integ, gath, rim, rim_recv, lip, lip_recv, held, chosen, arrived, thick, owner,
    load_sem, small_sem, send_sem, member_sem, recv_sem, round_sem,
):
    n_mem, n_ty, n_tx = sizes
    own, levels, rows, cols = u.shape
    quarter = rows // n_mem
    body = pl.ds(PAD, rows)
    mem, ty, tx = lax.axis_index("mem"), lax.axis_index("ty"), lax.axis_index("tx")
    me = ty * n_tx + tx
    east, west = lax.rem(tx + 1, n_tx), lax.rem(tx + n_tx - 1, n_tx)
    north, south = lax.rem(ty + 1, n_ty), lax.rem(ty + n_ty - 1, n_ty)
    scope = jax.named_scope

    homes, serve, hops, sides, reach = layout(n_ty, n_tx)

    def shift(*offsets):
        return sum(o[0] for o in offsets) % n_ty, sum(o[1] for o in offsets) % n_tx

    def place(*offsets, **at):
        a, b = shift(*offsets)
        return {"ty": lax.rem(ty + a, n_ty), "tx": lax.rem(tx + b, n_tx), **at}

    def member(i):
        return {"mem": lax.rem(mem + i, n_mem)}

    across, along = [place(o) for o in sides[:2]], [place(o) for o in sides[2:]]
    others = [member(i) for i in range(1, n_mem)]
    rounds = [across + along] * (reach - 1) + [others]

    def greet(sem, peers):
        for where in peers:
            pl.semaphore_signal(sem, inc=1, device_id=where, device_id_type=MESH)

    near = across + along + others
    barrier = pltpu.get_barrier_semaphore()
    greet(barrier, near)
    met = []

    def meet(more):
        for _ in range(more):
            n = len(met)
            if n == 0:
                pl.semaphore_wait(barrier, len(near))
            elif n <= len(rounds):
                pl.semaphore_wait(round_sem.at[n - 1], len(rounds[n - 1]))
            if n < len(rounds):
                greet(round_sem.at[n], rounds[n])
            met.append(n)

    def load(src, dst, sem):
        copy = pltpu.make_async_copy(src, dst, sem)
        copy.start()
        return copy

    loads = {}
    for m in range(own):
        loads["p", m] = load(p_hbm.at[m], p.at[m, :, body, :], load_sem.at[3 * m])
        loads["u", m] = load(u_hbm.at[m], u.at[m], load_sem.at[3 * m + 1])
        loads["v", m] = load(v_hbm.at[m], v.at[m, :, pl.ds(0, rows), :], load_sem.at[3 * m + 2])
        if m == 0:
            small = [load(thick_hbm, thick, small_sem.at[0]), load(owner_hbm, owner, small_sem.at[1])]
            loads["s"] = load(s_hbm, s, load_sem.at[3 * own])
    loads["w"] = load(w_hbm, w, load_sem.at[3 * own + 1])

    lane = lax.broadcasted_iota(jnp.int32, (rows, cols), 1)
    row = lax.broadcasted_iota(jnp.int32, (rows, cols), 0)
    lane8 = lax.broadcasted_iota(jnp.int32, (8, cols), 1)
    row8 = lax.broadcasted_iota(jnp.int32, (8, cols), 0)
    pair = lane >> 1
    even = (lane & 1) == 0
    is_first, is_last = lane == 0, lane == cols - 1
    is_edge = is_first | is_last
    zero = jnp.zeros((rows, cols), jnp.float32)
    blank = jnp.zeros((1, cols), jnp.float32)

    def to_west(x):
        return pltpu.roll(x, cols - 1, 1)

    def to_east(x):
        return pltpu.roll(x, 1, 1)

    def drain(ref, sem):
        pltpu.make_async_copy(ref, ref, sem).wait()

    def send(src, dst, kind, sem, where):
        pltpu.make_async_remote_copy(
            src_ref=src, dst_ref=dst, send_sem=send_sem.at[kind], recv_sem=sem, device_id=where, device_id_type=MESH
        ).start()

    def clear(k, c):
        for m in range(own):
            p[m, k, PAD - 1 : PAD, :] = blank
            p[m, k, PAD + rows : PAD + rows + 1, :] = blank
            v[m, k, rows : rows + 1, :] = blank
        sig[k, PAD - 1 : PAD, :] = blank
        sig[k, PAD + rows : PAD + rows + 1, :] = blank
        return c

    def pack(m):
        def one(k, packed):
            pk = p[m, k, body, :]
            ends = jnp.where(is_last, pk, u[m, k] - horiz_ratio * pk)
            return jnp.where(pair == k, pltpu.roll(ends, 2 * k + 1, 1), packed)

        edge[m] = unrolled(levels, one, zero, 50)

    def pack_rows(m):
        def one(k, c):
            first_row[m, pl.ds(k, 1), :] = v[m, k, 0:1, :] - horiz_ratio * p[m, k, PAD : PAD + 1, :]
            return c

        unrolled(levels, one, 0, 50)

    def pivots():
        def one(i, c):
            k = i + 1
            below, gprev, mass_below, value = c
            sk = s[k]
            hs[k] = horiz_ratio * sk
            vs[k] = vert_ratio * sk
            b = (vert_ratio * vert_ratio) * sk
            mass = thick[k] * sk
            r = 1.0 / (1.0 + b + below - below * gprev)
            gk = b * r
            bi = below * r
            value = (vert_ratio * (mass - mass_below)) * r + bi * value
            inv[k] = r
            binv[k] = bi
            g[k] = gk
            lam[k] = value
            return b, gk, mass, value

        s0 = s[0]
        hs[0] = horiz_ratio * s0
        vs[0] = vert_ratio * s0
        unrolled(levels - 1, one, ((vert_ratio * vert_ratio) * s0, zero, thick[0] * s0, zero))

    def adjoint():
        def weights(k, here, above, packed):
            mk = thick[k] - vert_ratio * (here - above)
            sk = (horiz_ratio * mk) * hs[k]
            mu[k] = mk
            sig[k, body, :] = sk
            sig_east[k] = to_west(sk)
            sig_west[k] = to_east(sk)
            alpha[k] = mk - 4.0 * sk
            return jnp.where(pair == k, pltpu.roll(sk, 2 * k + 1, 1), packed)

        def two(i, c):
            k = levels - 1 - i
            above, packed = c
            here = lam[k] + g[k] * above
            lam[k] = here
            return here, weights(k, here, above, packed)

        above, packed = unrolled(levels - 1, two, (zero, zero), 49)
        sig_edge[...] = weights(0, zero, above, packed)

    def diverge(m):
        def one(k, c):
            usum, vsum, psum = c
            pk, uk, vk = p[m, k, body, :], u[m, k], v[m, k, pl.ds(0, rows), :]
            around = to_east(pk) + (p[m, k, pl.ds(PAD - 1, rows), :] + p[m, k, pl.ds(PAD + 1, rows), :])
            div = (to_west(uk - horiz_ratio * pk) - uk) + (v[m, k, pl.ds(1, rows), :] - vk)
            u[m, k] = div - horiz_ratio * (around - 4.0 * pk)
            tk = thick[k]
            return usum + tk * uk, vsum + tk * vk, psum + tk * pk

        return unrolled(levels, one, (zero, zero, zero), 50)

    def forward(m):
        mine = edge[m]
        halo = jnp.where(
            even, -horiz_ratio * (edge_recv[m, 0] - mine), pltpu.roll(edge_recv[m, 1] - mine, cols - 2, 1))

        def level(k, rest):
            hk = pltpu.roll(halo, cols - 2 * k if not isinstance(k, int) or k > 0 else 0, 1)
            div = u[m, k] + jnp.where(is_edge, hk, 0.0)
            low = jnp.where(row8 == 0, -horiz_ratio * row_recv[m, 0, pl.ds(k, 1), :], 0.0)
            high = jnp.where(row8 == 7, row_recv[m, 1, pl.ds(k, 1), :], 0.0)
            div = jnp.concatenate([div[:8] + low, div[8 : rows - 8], div[rows - 8 :] + high], axis=0)
            e = hs[k] * div
            pa = p[m, k, body, :] - e
            part[m, k] = pa
            return pa, rest - mu[k] * e

        def one(i, c):
            k = i + 1
            pa_below, value, rest = c
            pa, rest = level(k, rest)
            rhs = w[m, i] - vert_ratio * (pa - pa_below)
            value = rhs * inv[k] + binv[k] * value
            w[m, i] = value
            return pa, value, rest

        pa, rest = level(0, zero)
        return unrolled(levels - 1, one, (pa, zero, rest), 49)[2]

    def backward(m, rest):
        def weigh(k, pk, packed, mass, rest, te, tw, tn, ts):
            p_rows[m, 0, pl.ds(k, 1), :] = pk[0:1]
            p_rows[m, 1, pl.ds(k, 1), :] = pk[rows - 1 : rows]
            return (
                jnp.where(pair == k, pltpu.roll(pk, 2 * k + 1, 1), packed),
                mass + thick[k] * pk,
                rest + alpha[k] * pk,
                te + sig_east[k] * pk,
                tw + sig_west[k] * pk,
                tn + sig[k, pl.ds(PAD + 1, rows), :] * pk,
                ts + sig[k, pl.ds(PAD - 1, rows), :] * pk,
            )

        def one(i, c):
            k = levels - 1 - i
            above, packed, mass, rest, *sides = c
            here = w[m, k - 1] + g[k] * above
            pk = part[m, k] - vs[k] * (above - here)
            return (here, *weigh(k, pk, packed, mass, rest + lam[k] * here, *sides))

        above, *sums = unrolled(levels - 1, one, (zero, zero, zero, rest, zero, zero, zero, zero), 49)
        packed, *sums = weigh(0, part[m, 0] - vs[0] * above, *sums)
        p_edge[m] = packed
        return sums

    def whole(m, usum, vsum, q, rest, te, tw, tn, ts):
        total = rest + jnp.where(is_first, 0.0, to_east(te)) + jnp.where(is_last, 0.0, to_west(tw))
        total = total + pltpu.roll(tn, 1, 0) + pltpu.roll(ts, rows - 1, 0)
        ue = usum - horiz_ratio * (q - jnp.where(is_first, 0.0, to_east(q)))
        vn = vsum - horiz_ratio * (q - jnp.where(row == 0, 0.0, pltpu.roll(q, 1, 0)))
        for r in range(n_mem):
            for f, x in enumerate((total, ue, vn)):
                integ[m, r, f] = x[r * quarter : (r + 1) * quarter]

    def send_whole(m):
        for n, h in reversed(list(enumerate(homes))):
            for i in range(0 if n else 1, n_mem):
                other = lax.rem(mem + i, n_mem)
                send(integ.at[m, other], gath.at[n * n_mem + mem, m], 4, recv_sem.at[2], place(h, mem=other))

    def rims(qs):
        sig_e, sig_w = pltpu.roll(sig_edge_recv[1], cols - 1, 1), pltpu.roll(sig_edge_recv[0], 1, 1)
        rims = zero
        for m in range(own):
            te = jnp.sum(jnp.where(even, sig_e * p_edge[m], 0.0), axis=1, keepdims=True)
            tw = jnp.sum(jnp.where(even, 0.0, sig_w * p_edge[m]), axis=1, keepdims=True)
            rims = jnp.where(lane == 2 * m, te, rims)
            rims = jnp.where(lane == 2 * m + 1, pltpu.roll(qs[m], 2 * m + 2, 1), rims)
            rims = jnp.where(lane == 2 * own + m, tw, rims)
        rims = jnp.where(lane < 4 * own, rims, 0.0)
        for r in range(n_mem):
            piece = rims[r * quarter : (r + 1) * quarter]
            piece = pltpu.roll(piece, 0, 1, stride=8, stride_axis=0)
            rim[r] = jnp.sum(piece, axis=0, keepdims=True)

    def send_rims():
        for n, h in reversed(list(enumerate(homes))):
            for i in range(n_mem):
                other = lax.rem(mem + i, n_mem)
                for kind in range(2):
                    send(
                        rim.at[other], rim_recv.at[n, kind, mem], 5, recv_sem.at[3],
                        place(h, sides[kind], mem=other))

    def lips(qs):
        for m in range(own):
            lip[m : m + 1, :] = jnp.sum(sig_rows[0] * p_rows[m, 1], axis=0, keepdims=True)
            lip[own + m : own + m + 1, :] = qs[m][rows - 1 : rows]
            lip[2 * own + m : 2 * own + m + 1, :] = jnp.sum(sig_rows[1] * p_rows[m, 0], axis=0, keepdims=True)

    goals = (0, n_mem - 1)
    kept = [sum(shift(h, sides[2 + kind]) == (0, 0) for h in homes) for kind in range(2)]

    def send_lips():
        for n, h in reversed(list(enumerate(homes))):
            for kind, goal in enumerate(goals):
                at = n * n_mem + mem
                if shift(h, sides[2 + kind]) != (0, 0):
                    send(lip, lip_recv.at[kind, at], 6, recv_sem.at[4], place(h, sides[2 + kind], mem=goal))
                    continue

                @pl.when(mem != goal)
                def _():
                    send(lip, lip_recv.at[kind, at], 8 + kind, recv_sem.at[4], {"mem": goal})

                @pl.when(mem == goal)
                def _():
                    lip_recv[kind, at] = lip[...]

    with scope("clear"):
        unrolled(levels, clear, 0, 10)
    for m in range(own):
        with scope(f"wait_p{m}"):
            loads["p", m].wait()
        if m == 0:
            with scope("wait_barrier"):
                meet(1)
        with scope(f"wait_u{m}"):
            send(p.at[m, :, PAD + rows - 1, :], row_recv.at[m, 0], 0, member_sem.at[m, 0], {"ty": north})
            loads["u", m].wait()
        with scope(f"pack{m}"):
            pack(m)
            send(edge.at[m], edge_recv.at[m, 0], 1, member_sem.at[m, 1], {"tx": east})
            send(edge.at[m], edge_recv.at[m, 1], 1, member_sem.at[m, 1], {"tx": west})
        with scope(f"wait_v{m}"):
            loads["v", m].wait()
        with scope(f"rows{m}"):
            pack_rows(m)
            send(first_row.at[m], row_recv.at[m, 1], 0, member_sem.at[m, 0], {"ty": south})
        if m == 0:
            with scope("wait_s"):
                loads["s"].wait()
                for copy in small:
                    copy.wait()
            with scope("pivots"):
                pivots()
    with scope("adjoint"):
        adjoint()
    with scope("send_sig"):
        send(sig_edge, sig_edge_recv.at[0], 2, recv_sem.at[0], {"tx": east})
        send(sig_edge, sig_edge_recv.at[1], 2, recv_sem.at[0], {"tx": west})
        send(sig.at[:, PAD, :], sig_rows.at[0], 3, recv_sem.at[1], {"ty": south})
        send(sig.at[:, PAD + rows - 1, :], sig_rows.at[1], 3, recv_sem.at[1], {"ty": north})
    sums = []
    for m in range(own):
        with scope(f"diverge{m}"):
            sums.append(diverge(m))
    with scope("meet0"):
        meet(len(rounds) - 1)

    qs = []
    for m in range(own):
        with scope(f"wait_edge{m}"):
            if m == 0:
                loads["w"].wait()
            drain(edge_recv.at[m], member_sem.at[m, 1])
        with scope(f"wait_row{m}"):
            drain(row_recv.at[m], member_sem.at[m, 0])
        with scope(f"forward{m}"):
            rest = forward(m)
        with scope(f"backward{m}"):
            mass, *rest = backward(m, rest)
        qs.append(sums[m][2] + mass)
        last = m == own - 1
        if m == 0:
            with scope("meet"):
                meet(len(rounds) + 1 - len(met))
        if last:
            with scope("wait_sig"):
                drain(sig_edge_recv, recv_sem.at[0])
                drain(sig_rows, recv_sem.at[1])
        with scope(f"sums{m}"):
            if last:
                rims(qs)
                lips(qs)
            whole(m, sums[m][0], sums[m][1], qs[m], *rest)
        with scope(f"send_sums{m}"):
            if last:
                send_rims()
                send_lips()
            send_whole(m)

    bottom = (row8[:quarter] == 0) & (mem == 0)
    top = (row8[:quarter] == quarter - 1) & (mem == n_mem - 1)
    with scope("wait_lip"):

        for kind, goal in enumerate(goals):

            @pl.when(mem == goal)
            def _():
                drain(lip_recv.at[kind, pl.ds(0, len(homes) * n_mem - kept[kind])], recv_sem.at[4])

    with scope("wait_rim"):
        drain(rim_recv, recv_sem.at[3])
    with scope("wait_mem"):
        drain(gath.at[pl.ds(0, len(homes) * n_mem - 1)], recv_sem.at[2])

    lane_q = lane[:quarter]

    column_of = lane_q - 8 * row[:quarter]

    def column(x, c):
        return jnp.sum(jnp.where(column_of == c, x, 0.0), axis=1, keepdims=True)

    def stats(n):
        fields = []
        for i in range(n_mem):
            other = lax.rem(mem + i, n_mem)
            from_west, from_east = rim_recv[n, 0, other], rim_recv[n, 1, other]
            from_south, from_north = lip_recv[0, n * n_mem + other], lip_recv[1, n * n_mem + other]
            for m in range(own):
                source = integ.at[m, mem] if n == 0 and i == 0 else gath.at[n * n_mem + other, m]
                total, ue, vn = (source[f] for f in range(3))
                te, qw = column(from_west, 2 * m), column(from_west, 2 * m + 1)
                tw = column(from_east, 2 * own + m)
                total = total + jnp.where(lane_q == 0, te, 0.0) + jnp.where(lane_q == cols - 1, tw, 0.0)
                total = total + jnp.where(bottom, from_south[m : m + 1], 0.0)
                total = total + jnp.where(top, from_north[2 * own + m : 2 * own + m + 1], 0.0)
                ue = ue + horiz_ratio * jnp.where(lane_q == 0, qw, 0.0)
                vn = vn + horiz_ratio * jnp.where(bottom, from_south[own + m : own + m + 1], 0.0)
                fields.append([total, ue, vn])

        members = len(fields)
        for f in range(3):
            total = fields[0][f]
            for one in fields[1:]:
                total = total + one[f]
            mean = total / members
            second = (fields[0][f] - mean) ** 2
            for one in fields[1:]:
                second = second + (one[f] - mean) ** 2
            held[n, f] = mean
            held[n, 3 + f] = second / (members - 1)

    def number(o):
        where = place(o)
        return where["ty"] * n_tx + where["tx"]

    def back(o):
        return (-o[0] % n_ty, -o[1] % n_tx)

    with scope("stats"):
        for n in range(len(homes)):
            stats(n)
        for i, hop in enumerate(hops):
            pick = jnp.int32(0)
            for n, h in enumerate(homes):
                if serve[shift(hop, h)] == n:
                    pick = jnp.where(owner[number(back(h))] == number(hop), n, pick)
            chosen[i] = held[pick]
            send(chosen.at[i], arrived.at[i], 7, recv_sem.at[5], place(hop))
        here, there, local = jnp.int32(0), jnp.int32(0), jnp.int32(0)
        for o, n in serve.items():
            found = owner[number(back(o))] == me
            hop = shift(o, back(homes[n]))
            if hop == (0, 0):
                here = jnp.where(found, n, here)
                local = jnp.where(found, 1, local)
            else:
                there = jnp.where(found, hops.index(hop), there)
    with scope("wait_all"):
        drain(arrived, recv_sem.at[5])
    with scope("finish"):
        out[0, 0] = jnp.where(local == 1, held[here], arrived[there])
        drain(row_recv, send_sem.at[0])
        drain(edge_recv, send_sem.at[1])
        drain(sig_edge_recv, send_sem.at[2])
        drain(sig_rows, send_sem.at[3])
        drain(gath.at[pl.ds(0, len(homes) * n_mem - 1)], send_sem.at[4])
        drain(rim_recv, send_sem.at[5])
        drain(lip_recv.at[0, pl.ds(0, 2 * len(homes) - kept[0] - kept[1])], send_sem.at[6])
        for kind, goal in enumerate(goals):
            if kept[kind]:

                @pl.when(mem != goal)
                def _():
                    drain(lip_recv.at[0, pl.ds(0, kept[kind])], send_sem.at[8 + kind])

        drain(arrived, send_sem.at[7])


def solution(mesh):
    n_mem, n_ty, n_tx = (mesh.shape[a] for a in ("mem", "ty", "tx"))
    homes, _, hops, _, reach = layout(n_ty, n_tx)

    def local(pressure, east_wind, north_wind, vertical_wind, sound_squared, thickness, owner_map):
        own, levels, rows, cols = pressure.shape
        quarter = rows // n_mem
        f32 = jnp.float32
        dma = pltpu.SemaphoreType.DMA

        def vmem(*shape):
            return pltpu.VMEM(shape, f32)

        return pl.pallas_call(
            functools.partial(kernel, (n_mem, n_ty, n_tx)),
            name="acoustic",
            out_shape=pltpu.VMEM((1, 1, 6, quarter, cols), f32),
            in_specs=[pl.BlockSpec(memory_space=pl.ANY)] * 7,
            out_specs=pl.BlockSpec(memory_space=pltpu.VMEM),
            scratch_shapes=[
                vmem(own, levels, rows + 2 * PAD, cols),
                vmem(own, levels, rows, cols),
                vmem(own, levels, rows + PAD, cols),
                vmem(own, levels - 1, rows, cols),
                vmem(levels, rows, cols),
                vmem(own, levels, rows, cols),
                *[vmem(levels, rows, cols)] * 8,
                vmem(levels, rows + 2 * PAD, cols),
                *[vmem(levels, rows, cols)] * 2,
                vmem(own, rows, cols),
                vmem(own, 2, rows, cols),
                vmem(own, levels, cols),
                vmem(own, 2, levels, cols),
                vmem(rows, cols),
                vmem(2, rows, cols),
                vmem(2, levels, cols),
                vmem(own, rows, cols),
                vmem(own, 2, levels, cols),
                vmem(own, n_mem, 3, quarter, cols),
                vmem(len(homes) * n_mem, own, 3, quarter, cols),
                vmem(n_mem, 1, cols),
                vmem(len(homes), 2, n_mem, 1, cols),
                vmem(-(-3 * own // 8) * 8, cols),
                vmem(2, len(homes) * n_mem, -(-3 * own // 8) * 8, cols),
                vmem(len(homes), 6, quarter, cols),
                vmem(len(hops), 6, quarter, cols),
                vmem(len(hops), 6, quarter, cols),
                pltpu.SMEM(thickness.shape, f32),
                pltpu.SMEM(owner_map.shape, jnp.int32),
                dma((3 * own + 2,)),
                dma((2,)),
                dma((10,)),
                dma((own, 2)),
                dma((6,)),
                pltpu.SemaphoreType.REGULAR((reach,)),
            ],
            compiler_params=pltpu.CompilerParams(collective_id=0, has_side_effects=True),
        )(pressure, east_wind, north_wind, vertical_wind, sound_squared, thickness, owner_map)

    field = P("mem", None, "ty", "tx")
    return jax.shard_map(
        local,
        mesh=mesh,
        in_specs=(field, field, field, field, P(None, "ty", "tx"), P(), P()),
        out_specs=P("ty", "tx", None, "mem", None),
        check_vma=False,
    )
```

```python
import functools

import jax
import jax.numpy as jnp
from jax import lax
from jax.experimental import pallas as pl
from jax.experimental.pallas import tpu as pltpu
from jax.sharding import PartitionSpec as P

MESH = pl.DeviceIdType.MESH
PAD = 8

horiz_ratio = 0.35
vert_ratio = 1.5


def unrolled(count, body, carry, most=7):
    trips = -(-count // most)
    width = count // trips
    first = count - trips * width

    def block(i, c):
        for j in range(width):
            c = body(first + i * width + j, c)
        return c

    for i in range(first):
        carry = body(i, carry)
    return lax.fori_loop(0, trips, block, carry)


def layout(n_ty, n_tx):
    homes = sorted({(0, 0), (n_ty // 2, 0)})

    def far(o, h):
        a, b = (o[0] - h[0]) % n_ty, (o[1] - h[1]) % n_tx
        return min(a, n_ty - a) + min(b, n_tx - b)

    serve, hops = {}, set()
    for o in ((a, b) for a in range(n_ty) for b in range(n_tx)):
        n = min(range(len(homes)), key=lambda i: far(o, homes[i]))
        serve[o] = n
        hops.add(((o[0] - homes[n][0]) % n_ty, (o[1] - homes[n][1]) % n_tx))
    sides = [(0, 1), (0, n_tx - 1), (1, 0), (n_ty - 1, 0)]
    reach = max(far(((a + c) % n_ty, (b + d) % n_tx), (0, 0)) for a, b in homes for c, d in sides + [(0, 0)])
    reach = max(reach, *(far(d, (0, 0)) for d in hops))
    return homes, serve, sorted(hops - {(0, 0)}, key=lambda d: (-far(d, (0, 0)), d)), sides, reach


def kernel(
    sizes,
    p_hbm, u_hbm, v_hbm, w_hbm, s_hbm, thick_hbm, owner_hbm,
    out,
    p, u, v, w, s, part, hs, vs, inv, binv, g, lam, mu, alpha, sig, sig_east, sig_west,
    edge, edge_recv, first_row, row_recv, sig_edge, sig_edge_recv, sig_rows, p_edge, p_rows,
    integ, gath, rim, rim_recv, lip, lip_recv, held, chosen, arrived, thick, owner,
    load_sem, small_sem, send_sem, member_sem, recv_sem, round_sem,
):
    n_mem, n_ty, n_tx = sizes
    own, levels, rows, cols = u.shape
    quarter = rows // n_mem
    body = pl.ds(PAD, rows)
    mem, ty, tx = lax.axis_index("mem"), lax.axis_index("ty"), lax.axis_index("tx")
    me = ty * n_tx + tx
    east, west = lax.rem(tx + 1, n_tx), lax.rem(tx + n_tx - 1, n_tx)
    north, south = lax.rem(ty + 1, n_ty), lax.rem(ty + n_ty - 1, n_ty)
    scope = jax.named_scope

    homes, serve, hops, sides, reach = layout(n_ty, n_tx)

    def shift(*offsets):
        return sum(o[0] for o in offsets) % n_ty, sum(o[1] for o in offsets) % n_tx

    def place(*offsets, **at):
        a, b = shift(*offsets)
        return {"ty": lax.rem(ty + a, n_ty), "tx": lax.rem(tx + b, n_tx), **at}

    def member(i):
        return {"mem": lax.rem(mem + i, n_mem)}

    across, along = [place(o) for o in sides[:2]], [place(o) for o in sides[2:]]
    others = [member(i) for i in range(1, n_mem)]
    rounds = [across + along] * (reach - 1) + [others]

    def greet(sem, peers):
        for where in peers:
            pl.semaphore_signal(sem, inc=1, device_id=where, device_id_type=MESH)

    near = across + along + others
    barrier = pltpu.get_barrier_semaphore()
    greet(barrier, near)
    met = []

    def meet(more):
        for _ in range(more):
            n = len(met)
            if n == 0:
                pl.semaphore_wait(barrier, len(near))
            elif n <= len(rounds):
                pl.semaphore_wait(round_sem.at[n - 1], len(rounds[n - 1]))
            if n < len(rounds):
                greet(round_sem.at[n], rounds[n])
            met.append(n)

    def load(src, dst, sem):
        copy = pltpu.make_async_copy(src, dst, sem)
        copy.start()
        return copy

    loads = {}
    for m in range(own):
        loads["p", m] = load(p_hbm.at[m], p.at[m, :, body, :], load_sem.at[3 * m])
        loads["u", m] = load(u_hbm.at[m], u.at[m], load_sem.at[3 * m + 1])
        loads["v", m] = load(v_hbm.at[m], v.at[m, :, pl.ds(0, rows), :], load_sem.at[3 * m + 2])
        if m == 0:
            small = [load(thick_hbm, thick, small_sem.at[0]), load(owner_hbm, owner, small_sem.at[1])]
            loads["s"] = load(s_hbm, s, load_sem.at[3 * own])
    loads["w"] = load(w_hbm, w, load_sem.at[3 * own + 1])

    lane = lax.broadcasted_iota(jnp.int32, (rows, cols), 1)
    row = lax.broadcasted_iota(jnp.int32, (rows, cols), 0)
    lane8 = lax.broadcasted_iota(jnp.int32, (8, cols), 1)
    row8 = lax.broadcasted_iota(jnp.int32, (8, cols), 0)
    column_of = lane - 8 * lax.rem(row, quarter)
    pair = lane >> 1
    even = (lane & 1) == 0
    is_first, is_last = lane == 0, lane == cols - 1
    is_edge = is_first | is_last
    zero = jnp.zeros((rows, cols), jnp.float32)
    blank = jnp.zeros((1, cols), jnp.float32)

    def to_west(x):
        return pltpu.roll(x, cols - 1, 1)

    def to_east(x):
        return pltpu.roll(x, 1, 1)

    def drain(ref, sem):
        pltpu.make_async_copy(ref, ref, sem).wait()

    def send(src, dst, kind, sem, where):
        pltpu.make_async_remote_copy(
            src_ref=src, dst_ref=dst, send_sem=send_sem.at[kind], recv_sem=sem, device_id=where, device_id_type=MESH
        ).start()

    def clear(k, c):
        for m in range(own):
            p[m, k, PAD - 1 : PAD, :] = blank
            p[m, k, PAD + rows : PAD + rows + 1, :] = blank
            v[m, k, rows : rows + 1, :] = blank
        sig[k, PAD - 1 : PAD, :] = blank
        sig[k, PAD + rows : PAD + rows + 1, :] = blank
        return c

    def pack(m):
        def one(k, packed):
            pk = p[m, k, body, :]
            ends = jnp.where(is_last, pk, u[m, k] - horiz_ratio * pk)
            return jnp.where(pair == k, pltpu.roll(ends, 2 * k + 1, 1), packed)

        edge[m] = unrolled(levels, one, zero, 50)

    def pack_rows(m):
        def one(k, c):
            first_row[m, pl.ds(k, 1), :] = v[m, k, 0:1, :] - horiz_ratio * p[m, k, PAD : PAD + 1, :]
            return c

        unrolled(levels, one, 0, 50)

    def pivots():
        def one(i, c):
            k = i + 1
            below, gprev, mass_below, value = c
            sk = s[k]
            hs[k] = horiz_ratio * sk
            vs[k] = vert_ratio * sk
            b = (vert_ratio * vert_ratio) * sk
            mass = thick[k] * sk
            r = 1.0 / (1.0 + b + below - below * gprev)
            gk = b * r
            bi = below * r
            value = (vert_ratio * (mass - mass_below)) * r + bi * value
            inv[k] = r
            binv[k] = bi
            g[k] = gk
            lam[k] = value
            return b, gk, mass, value

        s0 = s[0]
        hs[0] = horiz_ratio * s0
        vs[0] = vert_ratio * s0
        unrolled(levels - 1, one, ((vert_ratio * vert_ratio) * s0, zero, thick[0] * s0, zero))

    def adjoint():
        def weights(k, here, above, packed, lean):
            mk = thick[k] - vert_ratio * (here - above)
            sk = (horiz_ratio * mk) * hs[k]
            ak = mk - 4.0 * sk
            sig[k, body, :] = sk
            sig_east[k] = to_west(sk)
            sig_west[k] = to_east(sk)
            alpha[k] = ak
            mu[k] = mk + ak
            push = ak * vs[k]
            lam[k + 1] = lean - push
            return jnp.where(pair == k, pltpu.roll(sk, 2 * k + 1, 1), packed), here + push

        def two(i, c):
            k = levels - 1 - i
            above, packed, lean = c
            here = lam[k] + g[k] * above
            return here, *weights(k, here, above, packed, lean)

        above, packed, lean = unrolled(levels - 1, two, (zero, zero, zero), 49)
        sig_edge[...] = weights(0, zero, above, packed, lean)[0]

    def diverge(m):
        def one(k, c):
            usum, vsum, psum, rest = c
            pk, uk, vk = p[m, k, body, :], u[m, k], v[m, k, pl.ds(0, rows), :]
            around = to_east(pk) + (p[m, k, pl.ds(PAD - 1, rows), :] + p[m, k, pl.ds(PAD + 1, rows), :])
            div = (to_west(uk - horiz_ratio * pk) - uk) + (v[m, k, pl.ds(1, rows), :] - vk)
            u[m, k] = div - horiz_ratio * (around - 4.0 * pk)
            tk = thick[k]
            return usum + tk * uk, vsum + tk * vk, psum + tk * pk, rest + alpha[k] * pk

        return unrolled(levels, one, (zero, zero, zero, zero), 50)

    def forward(m, rest):
        mine = edge[m]
        halo = jnp.where(
            even, -horiz_ratio * (edge_recv[m, 0] - mine), pltpu.roll(edge_recv[m, 1] - mine, cols - 2, 1))

        def level(k, rest):
            hk = pltpu.roll(halo, cols - 2 * k if not isinstance(k, int) or k > 0 else 0, 1)
            div = u[m, k] + jnp.where(is_edge, hk, 0.0)
            low = jnp.where(row8 == 0, -horiz_ratio * row_recv[m, 0, pl.ds(k, 1), :], 0.0)
            high = jnp.where(row8 == 7, row_recv[m, 1, pl.ds(k, 1), :], 0.0)
            div = jnp.concatenate([div[:8] + low, div[8 : rows - 8], div[rows - 8 :] + high], axis=0)
            e = hs[k] * div
            pa = p[m, k, body, :] - e
            part[m, k] = pa
            return pa, rest - mu[k] * e

        def one(i, c):
            k = i + 1
            pa_below, value, rest = c
            pa, rest = level(k, rest)
            rhs = w[m, i] - vert_ratio * (pa - pa_below)
            value = rhs * inv[k] + binv[k] * value
            w[m, i] = value
            return pa, value, rest

        pa, rest = level(0, rest)
        return unrolled(levels - 1, one, (pa, zero, rest), 49)[2]

    def backward(m, rest):
        def weigh(k, pk, packed, mass, rest, te, tw, tn, ts):
            p_rows[m, 0, pl.ds(k, 1), :] = pk[0:1]
            p_rows[m, 1, pl.ds(k, 1), :] = pk[rows - 1 : rows]
            return (
                jnp.where(pair == k, pltpu.roll(pk, 2 * k + 1, 1), packed),
                mass + thick[k] * pk,
                rest,
                te + sig_east[k] * pk,
                tw + sig_west[k] * pk,
                tn + sig[k, pl.ds(PAD + 1, rows), :] * pk,
                ts + sig[k, pl.ds(PAD - 1, rows), :] * pk,
            )

        def one(i, c):
            k = levels - 1 - i
            above, packed, mass, rest, *sides = c
            here = w[m, k - 1] + g[k] * above
            pk = part[m, k] - vs[k] * (above - here)
            return (here, *weigh(k, pk, packed, mass, rest + lam[k] * here, *sides))

        above, *sums = unrolled(levels - 1, one, (zero, zero, zero, rest, zero, zero, zero, zero), 49)
        packed, *sums = weigh(0, part[m, 0] - vs[0] * above, *sums)
        p_edge[m] = packed
        return sums

    def whole(m, usum, vsum, q, rest, te, tw, tn, ts):
        total = rest + jnp.where(is_first, 0.0, to_east(te)) + jnp.where(is_last, 0.0, to_west(tw))
        total = total + pltpu.roll(tn, 1, 0) + pltpu.roll(ts, rows - 1, 0)
        ue = usum - horiz_ratio * (q - jnp.where(is_first, 0.0, to_east(q)))
        vn = vsum - horiz_ratio * (q - jnp.where(row == 0, 0.0, pltpu.roll(q, 1, 0)))
        for r in range(n_mem):
            for f, x in enumerate((total, ue, vn)):
                integ[m, r, f] = x[r * quarter : (r + 1) * quarter]

    def send_whole(m):
        for n, h in reversed(list(enumerate(homes))):
            for i in range(0 if n else 1, n_mem):
                other = lax.rem(mem + i, n_mem)
                send(integ.at[m, other], gath.at[n * n_mem + mem, m], 4, recv_sem.at[2], place(h, mem=other))

    def rims(qs):
        sig_e, sig_w = pltpu.roll(sig_edge_recv[1], cols - 1, 1), pltpu.roll(sig_edge_recv[0], 1, 1)
        rims = zero
        for m in range(own):
            te = jnp.sum(jnp.where(even, sig_e * p_edge[m], 0.0), axis=1, keepdims=True)
            tw = jnp.sum(jnp.where(even, 0.0, sig_w * p_edge[m]), axis=1, keepdims=True)
            q = jnp.sum(jnp.where(is_last, qs[m], 0.0), axis=1, keepdims=True)
            for c, x in ((2 * m, te), (2 * m + 1, q), (2 * own + m, tw)):
                rims = jnp.where(column_of == c, x, rims)
        for r in range(n_mem):
            rim[r] = jnp.sum(rims[r * quarter : (r + 1) * quarter], axis=0, keepdims=True)

    def send_rims():
        for n, h in reversed(list(enumerate(homes))):
            for i in range(n_mem):
                other = lax.rem(mem + i, n_mem)
                for kind in range(2):
                    send(
                        rim.at[other], rim_recv.at[n, kind, mem], 5, recv_sem.at[3],
                        place(h, sides[kind], mem=other))

    def lips(qs):
        for m in range(own):
            lip[m : m + 1, :] = jnp.sum(sig_rows[0] * p_rows[m, 1], axis=0, keepdims=True)
            lip[own + m : own + m + 1, :] = qs[m][rows - 1 : rows]
            lip[2 * own + m : 2 * own + m + 1, :] = jnp.sum(sig_rows[1] * p_rows[m, 0], axis=0, keepdims=True)

    goals = (0, n_mem - 1)
    kept = [sum(shift(h, sides[2 + kind]) == (0, 0) for h in homes) for kind in range(2)]

    def send_lips():
        for n, h in reversed(list(enumerate(homes))):
            for kind, goal in enumerate(goals):
                at = n * n_mem + mem
                if shift(h, sides[2 + kind]) != (0, 0):
                    send(lip, lip_recv.at[kind, at], 6, recv_sem.at[4], place(h, sides[2 + kind], mem=goal))
                    continue

                @pl.when(mem != goal)
                def _():
                    send(lip, lip_recv.at[kind, at], 8 + kind, recv_sem.at[4], {"mem": goal})

                @pl.when(mem == goal)
                def _():
                    lip_recv[kind, at] = lip[...]

    with scope("clear"):
        unrolled(levels, clear, 0, 10)
    for m in range(own):
        with scope(f"wait_p{m}"):
            loads["p", m].wait()
        with scope(f"wait_u{m}"):
            loads["u", m].wait()
        with scope(f"pack{m}"):
            pack(m)
        if m == 0:
            with scope("wait_barrier"):
                meet(1)
        with scope(f"send{m}"):
            send(edge.at[m], edge_recv.at[m, 0], 1, member_sem.at[m, 1], {"tx": east})
            send(edge.at[m], edge_recv.at[m, 1], 1, member_sem.at[m, 1], {"tx": west})
            send(p.at[m, :, PAD + rows - 1, :], row_recv.at[m, 0], 0, member_sem.at[m, 0], {"ty": north})
        with scope(f"wait_v{m}"):
            loads["v", m].wait()
        with scope(f"rows{m}"):
            pack_rows(m)
            send(first_row.at[m], row_recv.at[m, 1], 0, member_sem.at[m, 0], {"ty": south})
        if m == 0:
            with scope("wait_s"):
                loads["s"].wait()
                for copy in small:
                    copy.wait()
            with scope("pivots"):
                pivots()
    with scope("adjoint"):
        adjoint()
    with scope("send_sig"):
        send(sig_edge, sig_edge_recv.at[0], 2, recv_sem.at[0], {"tx": east})
        send(sig_edge, sig_edge_recv.at[1], 2, recv_sem.at[0], {"tx": west})
        send(sig.at[:, PAD, :], sig_rows.at[0], 3, recv_sem.at[1], {"ty": south})
        send(sig.at[:, PAD + rows - 1, :], sig_rows.at[1], 3, recv_sem.at[1], {"ty": north})
    sums = []
    for m in range(own):
        with scope(f"diverge{m}"):
            sums.append(diverge(m))
    with scope("meet0"):
        meet(len(rounds) - 1)

    qs = []
    for m in range(own):
        with scope(f"wait_edge{m}"):
            if m == 0:
                loads["w"].wait()
            drain(edge_recv.at[m], member_sem.at[m, 1])
        with scope(f"wait_row{m}"):
            drain(row_recv.at[m], member_sem.at[m, 0])
        with scope(f"forward{m}"):
            rest = forward(m, sums[m][3])
        with scope(f"backward{m}"):
            mass, *rest = backward(m, rest)
        qs.append(sums[m][2] + mass)
        last = m == own - 1
        if m == 0:
            with scope("meet"):
                meet(len(rounds) + 1 - len(met))
        if last:
            with scope("wait_sig"):
                drain(sig_edge_recv, recv_sem.at[0])
                drain(sig_rows, recv_sem.at[1])
        with scope(f"sums{m}"):
            if last:
                rims(qs)
                lips(qs)
            whole(m, sums[m][0], sums[m][1], qs[m], *rest)
        with scope(f"send_sums{m}"):
            if last:
                send_rims()
                send_lips()
            send_whole(m)

    bottom = (row8[:quarter] == 0) & (mem == 0)
    top = (row8[:quarter] == quarter - 1) & (mem == n_mem - 1)
    with scope("wait_lip"):

        for kind, goal in enumerate(goals):

            @pl.when(mem == goal)
            def _():
                drain(lip_recv.at[kind, pl.ds(0, len(homes) * n_mem - kept[kind])], recv_sem.at[4])

    with scope("wait_rim"):
        drain(rim_recv, recv_sem.at[3])
    with scope("wait_mem"):
        drain(gath.at[pl.ds(0, len(homes) * n_mem - 1)], recv_sem.at[2])

    lane_q = lane[:quarter]

    def column(x, c):
        return jnp.sum(jnp.where(column_of[:quarter] == c, x, 0.0), axis=1, keepdims=True)

    def stats(n):
        fields = []
        for i in range(n_mem):
            other = lax.rem(mem + i, n_mem)
            from_west, from_east = rim_recv[n, 0, other], rim_recv[n, 1, other]
            from_south, from_north = lip_recv[0, n * n_mem + other], lip_recv[1, n * n_mem + other]
            for m in range(own):
                source = integ.at[m, mem] if n == 0 and i == 0 else gath.at[n * n_mem + other, m]
                total, ue, vn = (source[f] for f in range(3))
                te, qw = column(from_west, 2 * m), column(from_west, 2 * m + 1)
                tw = column(from_east, 2 * own + m)
                total = total + jnp.where(lane_q == 0, te, 0.0) + jnp.where(lane_q == cols - 1, tw, 0.0)
                total = total + jnp.where(bottom, from_south[m : m + 1], 0.0)
                total = total + jnp.where(top, from_north[2 * own + m : 2 * own + m + 1], 0.0)
                ue = ue + horiz_ratio * jnp.where(lane_q == 0, qw, 0.0)
                vn = vn + horiz_ratio * jnp.where(bottom, from_south[own + m : own + m + 1], 0.0)
                fields.append([total, ue, vn])

        members = len(fields)
        for f in range(3):
            total = fields[0][f]
            for one in fields[1:]:
                total = total + one[f]
            mean = total / members
            second = (fields[0][f] - mean) ** 2
            for one in fields[1:]:
                second = second + (one[f] - mean) ** 2
            held[n, f] = mean
            held[n, 3 + f] = second / (members - 1)

    def number(o):
        where = place(o)
        return where["ty"] * n_tx + where["tx"]

    def back(o):
        return (-o[0] % n_ty, -o[1] % n_tx)

    with scope("stats"):
        for n in range(len(homes)):
            stats(n)
        for i, hop in enumerate(hops):
            pick = jnp.int32(0)
            for n, h in enumerate(homes):
                if serve[shift(hop, h)] == n:
                    pick = jnp.where(owner[number(back(h))] == number(hop), n, pick)
            chosen[i] = held[pick]
            send(chosen.at[i], arrived.at[i], 7, recv_sem.at[5], place(hop))
        here, there, local = jnp.int32(0), jnp.int32(0), jnp.int32(0)
        for o, n in serve.items():
            found = owner[number(back(o))] == me
            hop = shift(o, back(homes[n]))
            if hop == (0, 0):
                here = jnp.where(found, n, here)
                local = jnp.where(found, 1, local)
            else:
                there = jnp.where(found, hops.index(hop), there)
    with scope("wait_all"):
        drain(arrived, recv_sem.at[5])
    with scope("finish"):
        out[0, 0] = jnp.where(local == 1, held[here], arrived[there])
        drain(row_recv, send_sem.at[0])
        drain(edge_recv, send_sem.at[1])
        drain(sig_edge_recv, send_sem.at[2])
        drain(sig_rows, send_sem.at[3])
        drain(gath.at[pl.ds(0, len(homes) * n_mem - 1)], send_sem.at[4])
        drain(rim_recv, send_sem.at[5])
        drain(lip_recv.at[0, pl.ds(0, 2 * len(homes) - kept[0] - kept[1])], send_sem.at[6])
        for kind, goal in enumerate(goals):
            if kept[kind]:

                @pl.when(mem != goal)
                def _():
                    drain(lip_recv.at[0, pl.ds(0, kept[kind])], send_sem.at[8 + kind])

        drain(arrived, send_sem.at[7])


def solution(mesh):
    n_mem, n_ty, n_tx = (mesh.shape[a] for a in ("mem", "ty", "tx"))
    homes, _, hops, _, reach = layout(n_ty, n_tx)

    def local(pressure, east_wind, north_wind, vertical_wind, sound_squared, thickness, owner_map):
        own, levels, rows, cols = pressure.shape
        quarter = rows // n_mem
        f32 = jnp.float32
        dma = pltpu.SemaphoreType.DMA

        def vmem(*shape):
            return pltpu.VMEM(shape, f32)

        return pl.pallas_call(
            functools.partial(kernel, (n_mem, n_ty, n_tx)),
            name="acoustic",
            out_shape=pltpu.VMEM((1, 1, 6, quarter, cols), f32),
            in_specs=[pl.BlockSpec(memory_space=pl.ANY)] * 7,
            out_specs=pl.BlockSpec(memory_space=pltpu.VMEM),
            scratch_shapes=[
                vmem(own, levels, rows + 2 * PAD, cols),
                vmem(own, levels, rows, cols),
                vmem(own, levels, rows + PAD, cols),
                vmem(own, levels - 1, rows, cols),
                vmem(levels, rows, cols),
                vmem(own, levels, rows, cols),
                *[vmem(levels + 1, rows, cols)] * 8,
                vmem(levels, rows + 2 * PAD, cols),
                *[vmem(levels, rows, cols)] * 2,
                vmem(own, rows, cols),
                vmem(own, 2, rows, cols),
                vmem(own, levels, cols),
                vmem(own, 2, levels, cols),
                vmem(rows, cols),
                vmem(2, rows, cols),
                vmem(2, levels, cols),
                vmem(own, rows, cols),
                vmem(own, 2, levels, cols),
                vmem(own, n_mem, 3, quarter, cols),
                vmem(len(homes) * n_mem, own, 3, quarter, cols),
                vmem(n_mem, 1, cols),
                vmem(len(homes), 2, n_mem, 1, cols),
                vmem(-(-3 * own // 8) * 8, cols),
                vmem(2, len(homes) * n_mem, -(-3 * own // 8) * 8, cols),
                vmem(len(homes), 6, quarter, cols),
                vmem(len(hops), 6, quarter, cols),
                vmem(len(hops), 6, quarter, cols),
                pltpu.SMEM(thickness.shape, f32),
                pltpu.SMEM(owner_map.shape, jnp.int32),
                dma((3 * own + 2,)),
                dma((2,)),
                dma((10,)),
                dma((own, 2)),
                dma((6,)),
                pltpu.SemaphoreType.REGULAR((reach,)),
            ],
            compiler_params=pltpu.CompilerParams(collective_id=0, has_side_effects=True),
        )(pressure, east_wind, north_wind, vertical_wind, sound_squared, thickness, owner_map)

    field = P("mem", None, "ty", "tx")
    return jax.shard_map(
        local,
        mesh=mesh,
        in_specs=(field, field, field, field, P(None, "ty", "tx"), P(), P()),
        out_specs=P("ty", "tx", None, "mem", None),
        check_vma=False,
    )
```

```python
import functools

import jax
import jax.numpy as jnp
from jax import lax
from jax.experimental import pallas as pl
from jax.experimental.pallas import tpu as pltpu
from jax.sharding import PartitionSpec as P

MESH = pl.DeviceIdType.MESH
PAD = 8

horiz_ratio = 0.35
vert_ratio = 1.5


def unrolled(count, body, carry, most=7):
    trips = -(-count // most)
    width = count // trips
    first = count - trips * width

    def block(i, c):
        for j in range(width):
            c = body(first + i * width + j, c)
        return c

    for i in range(first):
        carry = body(i, carry)
    return lax.fori_loop(0, trips, block, carry)


def layout(n_ty, n_tx):
    homes = sorted({(0, 0), (n_ty // 2, 0)})

    def far(o, h):
        a, b = (o[0] - h[0]) % n_ty, (o[1] - h[1]) % n_tx
        return min(a, n_ty - a) + min(b, n_tx - b)

    serve, hops = {}, set()
    for o in ((a, b) for a in range(n_ty) for b in range(n_tx)):
        n = min(range(len(homes)), key=lambda i: far(o, homes[i]))
        serve[o] = n
        hops.add(((o[0] - homes[n][0]) % n_ty, (o[1] - homes[n][1]) % n_tx))
    sides = [(0, 1), (0, n_tx - 1), (1, 0), (n_ty - 1, 0)]
    reach = max(far(((a + c) % n_ty, (b + d) % n_tx), (0, 0)) for a, b in homes for c, d in sides + [(0, 0)])
    reach = max(reach, *(far(d, (0, 0)) for d in hops))
    return homes, serve, sorted(hops - {(0, 0)}, key=lambda d: (-far(d, (0, 0)), d)), sides, reach


def kernel(
    sizes,
    p_hbm, u_hbm, v_hbm, w_hbm, s_hbm, thick_hbm, owner_hbm,
    out,
    p, u, v, w, s, part, hs, vs, inv, binv, g, lam, mu, alpha, sig, sig_east, sig_west,
    edge, edge_recv, first_row, row_recv, sig_edge, sig_edge_recv, sig_rows, p_edge, p_rows,
    integ, gath, rim, rim_recv, lip, lip_recv, held, chosen, arrived, thick, owner,
    load_sem, small_sem, send_sem, member_sem, recv_sem, round_sem,
):
    n_mem, n_ty, n_tx = sizes
    own, levels, rows, cols = u.shape
    quarter = rows // n_mem
    body = pl.ds(PAD, rows)
    mem, ty, tx = lax.axis_index("mem"), lax.axis_index("ty"), lax.axis_index("tx")
    me = ty * n_tx + tx
    east, west = lax.rem(tx + 1, n_tx), lax.rem(tx + n_tx - 1, n_tx)
    north, south = lax.rem(ty + 1, n_ty), lax.rem(ty + n_ty - 1, n_ty)
    scope = jax.named_scope

    homes, serve, hops, sides, reach = layout(n_ty, n_tx)

    def shift(*offsets):
        return sum(o[0] for o in offsets) % n_ty, sum(o[1] for o in offsets) % n_tx

    def place(*offsets, **at):
        a, b = shift(*offsets)
        return {"ty": lax.rem(ty + a, n_ty), "tx": lax.rem(tx + b, n_tx), **at}

    def member(i):
        return {"mem": lax.rem(mem + i, n_mem)}

    across, along = [place(o) for o in sides[:2]], [place(o) for o in sides[2:]]
    others = [member(i) for i in range(1, n_mem)]
    rounds = [across + along] * (reach - 1) + [others]

    def greet(sem, peers):
        for where in peers:
            pl.semaphore_signal(sem, inc=1, device_id=where, device_id_type=MESH)

    near = across + along + others
    barrier = pltpu.get_barrier_semaphore()
    greet(barrier, near)
    met = []

    def meet(more):
        for _ in range(more):
            n = len(met)
            if n == 0:
                pl.semaphore_wait(barrier, len(near))
            elif n <= len(rounds):
                pl.semaphore_wait(round_sem.at[n - 1], len(rounds[n - 1]))
            if n < len(rounds):
                greet(round_sem.at[n], rounds[n])
            met.append(n)

    def load(src, dst, sem):
        copy = pltpu.make_async_copy(src, dst, sem)
        copy.start()
        return copy

    loads = {}
    for m in range(own):
        loads["p", m] = load(p_hbm.at[m], p.at[m, :, body, :], load_sem.at[3 * m])
        loads["u", m] = load(u_hbm.at[m], u.at[m], load_sem.at[3 * m + 1])
        loads["v", m] = load(v_hbm.at[m], v.at[m, :, pl.ds(0, rows), :], load_sem.at[3 * m + 2])
        if m == 0:
            small = [load(thick_hbm, thick, small_sem.at[0]), load(owner_hbm, owner, small_sem.at[1])]
            loads["s"] = load(s_hbm, s, load_sem.at[3 * own])
    loads["w"] = load(w_hbm, w, load_sem.at[3 * own + 1])

    lane = lax.broadcasted_iota(jnp.int32, (rows, cols), 1)
    row = lax.broadcasted_iota(jnp.int32, (rows, cols), 0)
    lane8 = lax.broadcasted_iota(jnp.int32, (8, cols), 1)
    row8 = lax.broadcasted_iota(jnp.int32, (8, cols), 0)
    column_of = lane - 8 * lax.rem(row, quarter)
    pair = lane >> 1
    even = (lane & 1) == 0
    is_first, is_last = lane == 0, lane == cols - 1
    is_edge = is_first | is_last
    zero = jnp.zeros((rows, cols), jnp.float32)
    blank = jnp.zeros((1, cols), jnp.float32)

    def to_west(x):
        return pltpu.roll(x, cols - 1, 1)

    def to_east(x):
        return pltpu.roll(x, 1, 1)

    def drain(ref, sem):
        pltpu.make_async_copy(ref, ref, sem).wait()

    def send(src, dst, kind, sem, where):
        pltpu.make_async_remote_copy(
            src_ref=src, dst_ref=dst, send_sem=send_sem.at[kind], recv_sem=sem, device_id=where, device_id_type=MESH
        ).start()

    def clear(k, c):
        for m in range(own):
            p[m, k, PAD - 1 : PAD, :] = blank
            p[m, k, PAD + rows : PAD + rows + 1, :] = blank
            v[m, k, rows : rows + 1, :] = blank
        sig[k, PAD - 1 : PAD, :] = blank
        sig[k, PAD + rows : PAD + rows + 1, :] = blank
        return c

    def pack(m):
        def one(k, packed):
            pk = p[m, k, body, :]
            ends = jnp.where(is_last, pk, u[m, k] - horiz_ratio * pk)
            return jnp.where(pair == k, pltpu.roll(ends, 2 * k + 1, 1), packed)

        edge[m] = unrolled(levels, one, zero, 50)

    def pack_rows(m):
        def one(k, c):
            first_row[m, pl.ds(k, 1), :] = v[m, k, 0:1, :] - horiz_ratio * p[m, k, PAD : PAD + 1, :]
            return c

        unrolled(levels, one, 0, 50)

    def pivots():
        def one(i, c):
            k = i + 1
            below, gprev, mass_below, value = c
            sk = s[k]
            hs[k] = horiz_ratio * sk
            vs[k] = vert_ratio * sk
            b = (vert_ratio * vert_ratio) * sk
            mass = thick[k] * sk
            r = 1.0 / (1.0 + b + below - below * gprev)
            gk = b * r
            bi = below * r
            value = (vert_ratio * (mass - mass_below)) * r + bi * value
            inv[k] = r
            binv[k] = bi
            g[k] = gk
            lam[k] = value
            return b, gk, mass, value

        s0 = s[0]
        hs[0] = horiz_ratio * s0
        vs[0] = vert_ratio * s0
        unrolled(levels - 1, one, ((vert_ratio * vert_ratio) * s0, zero, thick[0] * s0, zero))

    def adjoint():
        def weights(k, here, above, packed, lean):
            mk = thick[k] - vert_ratio * (here - above)
            sk = (horiz_ratio * mk) * hs[k]
            ak = mk - 4.0 * sk
            sig[k, body, :] = sk
            sig_east[k] = to_west(sk)
            sig_west[k] = to_east(sk)
            alpha[k] = ak
            mu[k] = mk + ak
            push = ak * vs[k]
            lam[k + 1] = lean - push
            return jnp.where(pair == k, pltpu.roll(sk, 2 * k + 1, 1), packed), here + push

        def two(i, c):
            k = levels - 1 - i
            above, packed, lean = c
            here = lam[k] + g[k] * above
            return here, *weights(k, here, above, packed, lean)

        above, packed, lean = unrolled(levels - 1, two, (zero, zero, zero), 49)
        sig_edge[...] = weights(0, zero, above, packed, lean)[0]

    def diverge(m):
        def one(k, c):
            usum, vsum, psum, rest = c
            pk, uk, vk = p[m, k, body, :], u[m, k], v[m, k, pl.ds(0, rows), :]
            around = to_east(pk) + (p[m, k, pl.ds(PAD - 1, rows), :] + p[m, k, pl.ds(PAD + 1, rows), :])
            div = (to_west(uk - horiz_ratio * pk) - uk) + (v[m, k, pl.ds(1, rows), :] - vk)
            u[m, k] = div - horiz_ratio * (around - 4.0 * pk)
            tk = thick[k]
            return usum + tk * uk, vsum + tk * vk, psum + tk * pk, rest + alpha[k] * pk

        return unrolled(levels, one, (zero, zero, zero, zero), 50)

    def forward(m, rest):
        mine = edge[m]
        halo = jnp.where(
            even, -horiz_ratio * (edge_recv[m, 0] - mine), pltpu.roll(edge_recv[m, 1] - mine, cols - 2, 1))

        def level(k, rest):
            hk = pltpu.roll(halo, cols - 2 * k if not isinstance(k, int) or k > 0 else 0, 1)
            div = u[m, k] + jnp.where(is_edge, hk, 0.0)
            low = jnp.where(row8 == 0, -horiz_ratio * row_recv[m, 0, pl.ds(k, 1), :], 0.0)
            high = jnp.where(row8 == 7, row_recv[m, 1, pl.ds(k, 1), :], 0.0)
            div = jnp.concatenate([div[:8] + low, div[8 : rows - 8], div[rows - 8 :] + high], axis=0)
            e = hs[k] * div
            pa = p[m, k, body, :] - e
            part[m, k] = pa
            return pa, rest - mu[k] * e

        def one(i, c):
            k = i + 1
            pa_below, value, rest = c
            pa, rest = level(k, rest)
            rhs = w[m, i] - vert_ratio * (pa - pa_below)
            value = rhs * inv[k] + binv[k] * value
            w[m, i] = value
            return pa, value, rest

        pa, rest = level(0, rest)
        return unrolled(levels - 1, one, (pa, zero, rest), 49)[2]

    def backward(m, rest):
        def weigh(k, pk, packed, mass, rest, te, tw, tn, ts):
            p_rows[m, 0, pl.ds(k, 1), :] = pk[0:1]
            p_rows[m, 1, pl.ds(k, 1), :] = pk[rows - 1 : rows]
            return (
                jnp.where(pair == k, pltpu.roll(pk, 2 * k + 1, 1), packed),
                mass + thick[k] * pk,
                rest,
                te + sig_east[k] * pk,
                tw + sig_west[k] * pk,
                tn + sig[k, pl.ds(PAD + 1, rows), :] * pk,
                ts + sig[k, pl.ds(PAD - 1, rows), :] * pk,
            )

        def one(i, c):
            k = levels - 1 - i
            above, packed, mass, rest, *sides = c
            here = w[m, k - 1] + g[k] * above
            pk = part[m, k] - vs[k] * (above - here)
            return (here, *weigh(k, pk, packed, mass, rest + lam[k] * here, *sides))

        above, *sums = unrolled(levels - 1, one, (zero, zero, zero, rest, zero, zero, zero, zero), 49)
        packed, *sums = weigh(0, part[m, 0] - vs[0] * above, *sums)
        p_edge[m] = packed
        return sums

    def whole(m, usum, vsum, q, rest, te, tw, tn, ts):
        total = rest + jnp.where(is_first, 0.0, to_east(te)) + jnp.where(is_last, 0.0, to_west(tw))
        total = total + pltpu.roll(tn, 1, 0) + pltpu.roll(ts, rows - 1, 0)
        ue = usum - horiz_ratio * (q - jnp.where(is_first, 0.0, to_east(q)))
        vn = vsum - horiz_ratio * (q - jnp.where(row == 0, 0.0, pltpu.roll(q, 1, 0)))
        for r in range(n_mem):
            for f, x in enumerate((total, ue, vn)):
                integ[m, r, f] = x[r * quarter : (r + 1) * quarter]

    def send_whole(m):
        for n, h in reversed(list(enumerate(homes))):
            for i in range(0 if n else 1, n_mem):
                other = lax.rem(mem + i, n_mem)
                send(integ.at[m, other], gath.at[n * n_mem + mem, m], 4, recv_sem.at[2], place(h, mem=other))

    def rims(qs):
        sig_e, sig_w = pltpu.roll(sig_edge_recv[1], cols - 1, 1), pltpu.roll(sig_edge_recv[0], 1, 1)
        rims = zero
        for m in range(own):
            te = jnp.sum(jnp.where(even, sig_e * p_edge[m], 0.0), axis=1, keepdims=True)
            tw = jnp.sum(jnp.where(even, 0.0, sig_w * p_edge[m]), axis=1, keepdims=True)
            q = jnp.sum(jnp.where(is_last, qs[m], 0.0), axis=1, keepdims=True)
            for c, x in ((2 * m, te), (2 * m + 1, q), (2 * own + m, tw)):
                rims = jnp.where(column_of == c, x, rims)
        for r in range(n_mem):
            rim[r] = jnp.sum(rims[r * quarter : (r + 1) * quarter], axis=0, keepdims=True)

    def send_rims():
        for n, h in reversed(list(enumerate(homes))):
            for goal in sorted(range(n_mem), key=lambda q: (q % 2, q)):
                for kind in range(2):
                    send(
                        rim.at[goal], rim_recv.at[n, kind, mem], 5, recv_sem.at[3],
                        place(h, sides[kind], mem=goal))

    def lips(qs):
        for m in range(own):
            lip[m : m + 1, :] = jnp.sum(sig_rows[0] * p_rows[m, 1], axis=0, keepdims=True)
            lip[own + m : own + m + 1, :] = qs[m][rows - 1 : rows]
            lip[2 * own + m : 2 * own + m + 1, :] = jnp.sum(sig_rows[1] * p_rows[m, 0], axis=0, keepdims=True)

    goals = (0, n_mem - 1)
    kept = [sum(shift(h, sides[2 + kind]) == (0, 0) for h in homes) for kind in range(2)]

    def send_lips():
        for n, h in reversed(list(enumerate(homes))):
            for kind, goal in enumerate(goals):
                at = n * n_mem + mem
                if shift(h, sides[2 + kind]) != (0, 0):
                    send(lip, lip_recv.at[kind, at], 6, recv_sem.at[4], place(h, sides[2 + kind], mem=goal))
                    continue

                @pl.when(mem != goal)
                def _():
                    send(lip, lip_recv.at[kind, at], 8 + kind, recv_sem.at[4], {"mem": goal})

                @pl.when(mem == goal)
                def _():
                    lip_recv[kind, at] = lip[...]

    with scope("clear"):
        unrolled(levels, clear, 0, 10)
    for m in range(own):
        with scope(f"wait_p{m}"):
            loads["p", m].wait()
        with scope(f"wait_u{m}"):
            loads["u", m].wait()
        with scope(f"pack{m}"):
            pack(m)
        if m == 0:
            with scope("wait_barrier"):
                meet(1)
        with scope(f"send{m}"):
            send(p.at[m, :, PAD + rows - 1, :], row_recv.at[m, 0], 0, member_sem.at[m, 0], {"ty": north})
            send(edge.at[m], edge_recv.at[m, 0], 1, member_sem.at[m, 1], {"tx": east})
            send(edge.at[m], edge_recv.at[m, 1], 1, member_sem.at[m, 1], {"tx": west})
        with scope(f"wait_v{m}"):
            loads["v", m].wait()
        with scope(f"rows{m}"):
            pack_rows(m)
            send(first_row.at[m], row_recv.at[m, 1], 0, member_sem.at[m, 0], {"ty": south})
        if m == 0:
            with scope("wait_s"):
                loads["s"].wait()
                for copy in small:
                    copy.wait()
            with scope("pivots"):
                pivots()
    with scope("adjoint"):
        adjoint()
    with scope("send_sig"):
        send(sig_edge, sig_edge_recv.at[0], 2, recv_sem.at[0], {"tx": east})
        send(sig_edge, sig_edge_recv.at[1], 2, recv_sem.at[0], {"tx": west})
        send(sig.at[:, PAD, :], sig_rows.at[0], 3, recv_sem.at[1], {"ty": south})
        send(sig.at[:, PAD + rows - 1, :], sig_rows.at[1], 3, recv_sem.at[1], {"ty": north})
    sums = []
    for m in range(own):
        with scope(f"diverge{m}"):
            sums.append(diverge(m))
    with scope("meet0"):
        meet(len(rounds) - 1)

    qs = []
    for m in range(own):
        with scope(f"wait_edge{m}"):
            if m == 0:
                loads["w"].wait()
            drain(edge_recv.at[m], member_sem.at[m, 1])
        with scope(f"wait_row{m}"):
            drain(row_recv.at[m], member_sem.at[m, 0])
        with scope(f"forward{m}"):
            rest = forward(m, sums[m][3])
        with scope(f"backward{m}"):
            mass, *rest = backward(m, rest)
        qs.append(sums[m][2] + mass)
        last = m == own - 1
        if m == 0:
            with scope("meet"):
                meet(len(rounds) + 1 - len(met))
        if last:
            with scope("wait_sig"):
                drain(sig_edge_recv, recv_sem.at[0])
                drain(sig_rows, recv_sem.at[1])
        with scope(f"sums{m}"):
            if last:
                rims(qs)
                send_rims()
                lips(qs)
            whole(m, sums[m][0], sums[m][1], qs[m], *rest)
        with scope(f"send_sums{m}"):
            if last:
                send_lips()
            send_whole(m)

    bottom = (row8[:quarter] == 0) & (mem == 0)
    top = (row8[:quarter] == quarter - 1) & (mem == n_mem - 1)
    with scope("wait_lip"):

        for kind, goal in enumerate(goals):

            @pl.when(mem == goal)
            def _():
                drain(lip_recv.at[kind, pl.ds(0, len(homes) * n_mem - kept[kind])], recv_sem.at[4])

    with scope("wait_rim"):
        drain(rim_recv, recv_sem.at[3])
    with scope("wait_mem"):
        drain(gath.at[pl.ds(0, len(homes) * n_mem - 1)], recv_sem.at[2])

    lane_q = lane[:quarter]

    def column(x, c):
        return jnp.sum(jnp.where(column_of[:quarter] == c, x, 0.0), axis=1, keepdims=True)

    def stats(n):
        fields = []
        for i in range(n_mem):
            other = lax.rem(mem + i, n_mem)
            from_west, from_east = rim_recv[n, 0, other], rim_recv[n, 1, other]
            from_south, from_north = lip_recv[0, n * n_mem + other], lip_recv[1, n * n_mem + other]
            for m in range(own):
                source = integ.at[m, mem] if n == 0 and i == 0 else gath.at[n * n_mem + other, m]
                total, ue, vn = (source[f] for f in range(3))
                te, qw = column(from_west, 2 * m), column(from_west, 2 * m + 1)
                tw = column(from_east, 2 * own + m)
                total = total + jnp.where(lane_q == 0, te, 0.0) + jnp.where(lane_q == cols - 1, tw, 0.0)
                total = total + jnp.where(bottom, from_south[m : m + 1], 0.0)
                total = total + jnp.where(top, from_north[2 * own + m : 2 * own + m + 1], 0.0)
                ue = ue + horiz_ratio * jnp.where(lane_q == 0, qw, 0.0)
                vn = vn + horiz_ratio * jnp.where(bottom, from_south[own + m : own + m + 1], 0.0)
                fields.append([total, ue, vn])

        members = len(fields)
        for f in range(3):
            total = fields[0][f]
            for one in fields[1:]:
                total = total + one[f]
            mean = total / members
            second = (fields[0][f] - mean) ** 2
            for one in fields[1:]:
                second = second + (one[f] - mean) ** 2
            held[n, f] = mean
            held[n, 3 + f] = second / (members - 1)

    def number(o):
        where = place(o)
        return where["ty"] * n_tx + where["tx"]

    def back(o):
        return (-o[0] % n_ty, -o[1] % n_tx)

    with scope("stats"):
        for n in range(len(homes)):
            stats(n)
        for i, hop in enumerate(hops):
            pick = jnp.int32(0)
            for n, h in enumerate(homes):
                if serve[shift(hop, h)] == n:
                    pick = jnp.where(owner[number(back(h))] == number(hop), n, pick)
            chosen[i] = held[pick]
            send(chosen.at[i], arrived.at[i], 7, recv_sem.at[5], place(hop))
        here, there, local = jnp.int32(0), jnp.int32(0), jnp.int32(0)
        for o, n in serve.items():
            found = owner[number(back(o))] == me
            hop = shift(o, back(homes[n]))
            if hop == (0, 0):
                here = jnp.where(found, n, here)
                local = jnp.where(found, 1, local)
            else:
                there = jnp.where(found, hops.index(hop), there)
    with scope("wait_all"):
        drain(arrived, recv_sem.at[5])
    with scope("finish"):
        out[0, 0] = jnp.where(local == 1, held[here], arrived[there])
        drain(row_recv, send_sem.at[0])
        drain(edge_recv, send_sem.at[1])
        drain(sig_edge_recv, send_sem.at[2])
        drain(sig_rows, send_sem.at[3])
        drain(gath.at[pl.ds(0, len(homes) * n_mem - 1)], send_sem.at[4])
        drain(rim_recv, send_sem.at[5])
        drain(lip_recv.at[0, pl.ds(0, 2 * len(homes) - kept[0] - kept[1])], send_sem.at[6])
        for kind, goal in enumerate(goals):
            if kept[kind]:

                @pl.when(mem != goal)
                def _():
                    drain(lip_recv.at[0, pl.ds(0, kept[kind])], send_sem.at[8 + kind])

        drain(arrived, send_sem.at[7])


def solution(mesh):
    n_mem, n_ty, n_tx = (mesh.shape[a] for a in ("mem", "ty", "tx"))
    homes, _, hops, _, reach = layout(n_ty, n_tx)

    def local(pressure, east_wind, north_wind, vertical_wind, sound_squared, thickness, owner_map):
        own, levels, rows, cols = pressure.shape
        quarter = rows // n_mem
        f32 = jnp.float32
        dma = pltpu.SemaphoreType.DMA

        def vmem(*shape):
            return pltpu.VMEM(shape, f32)

        return pl.pallas_call(
            functools.partial(kernel, (n_mem, n_ty, n_tx)),
            name="acoustic",
            out_shape=pltpu.VMEM((1, 1, 6, quarter, cols), f32),
            in_specs=[pl.BlockSpec(memory_space=pl.ANY)] * 7,
            out_specs=pl.BlockSpec(memory_space=pltpu.VMEM),
            scratch_shapes=[
                vmem(own, levels, rows + 2 * PAD, cols),
                vmem(own, levels, rows, cols),
                vmem(own, levels, rows + PAD, cols),
                vmem(own, levels - 1, rows, cols),
                vmem(levels, rows, cols),
                vmem(own, levels, rows, cols),
                *[vmem(levels + 1, rows, cols)] * 8,
                vmem(levels, rows + 2 * PAD, cols),
                *[vmem(levels, rows, cols)] * 2,
                vmem(own, rows, cols),
                vmem(own, 2, rows, cols),
                vmem(own, levels, cols),
                vmem(own, 2, levels, cols),
                vmem(rows, cols),
                vmem(2, rows, cols),
                vmem(2, levels, cols),
                vmem(own, rows, cols),
                vmem(own, 2, levels, cols),
                vmem(own, n_mem, 3, quarter, cols),
                vmem(len(homes) * n_mem, own, 3, quarter, cols),
                vmem(n_mem, 1, cols),
                vmem(len(homes), 2, n_mem, 1, cols),
                vmem(-(-3 * own // 8) * 8, cols),
                vmem(2, len(homes) * n_mem, -(-3 * own // 8) * 8, cols),
                vmem(len(homes), 6, quarter, cols),
                vmem(len(hops), 6, quarter, cols),
                vmem(len(hops), 6, quarter, cols),
                pltpu.SMEM(thickness.shape, f32),
                pltpu.SMEM(owner_map.shape, jnp.int32),
                dma((3 * own + 2,)),
                dma((2,)),
                dma((10,)),
                dma((own, 2)),
                dma((6,)),
                pltpu.SemaphoreType.REGULAR((reach,)),
            ],
            compiler_params=pltpu.CompilerParams(collective_id=0, has_side_effects=True),
        )(pressure, east_wind, north_wind, vertical_wind, sound_squared, thickness, owner_map)

    field = P("mem", None, "ty", "tx")
    return jax.shard_map(
        local,
        mesh=mesh,
        in_specs=(field, field, field, field, P(None, "ty", "tx"), P(), P()),
        out_specs=P("ty", "tx", None, "mem", None),
        check_vma=False,
    )
```

```python
import functools

import jax
import jax.numpy as jnp
from jax import lax
from jax.experimental import pallas as pl
from jax.experimental.pallas import tpu as pltpu
from jax.sharding import PartitionSpec as P

MESH = pl.DeviceIdType.MESH
PAD = 8

horiz_ratio = 0.35
vert_ratio = 1.5


def unrolled(count, body, carry, most=7):
    trips = -(-count // most)
    width = count // trips
    first = count - trips * width

    def block(i, c):
        for j in range(width):
            c = body(first + i * width + j, c)
        return c

    for i in range(first):
        carry = body(i, carry)
    return lax.fori_loop(0, trips, block, carry)


def layout(n_ty, n_tx):
    homes = sorted({(0, 0), (n_ty // 2, 0)})

    def far(o, h):
        a, b = (o[0] - h[0]) % n_ty, (o[1] - h[1]) % n_tx
        return min(a, n_ty - a) + min(b, n_tx - b)

    serve, hops = {}, set()
    for o in ((a, b) for a in range(n_ty) for b in range(n_tx)):
        n = min(range(len(homes)), key=lambda i: far(o, homes[i]))
        serve[o] = n
        hops.add(((o[0] - homes[n][0]) % n_ty, (o[1] - homes[n][1]) % n_tx))
    sides = [(0, 1), (0, n_tx - 1), (1, 0), (n_ty - 1, 0)]
    reach = max(far(((a + c) % n_ty, (b + d) % n_tx), (0, 0)) for a, b in homes for c, d in sides + [(0, 0)])
    reach = max(reach, *(far(d, (0, 0)) for d in hops))
    return homes, serve, sorted(hops - {(0, 0)}, key=lambda d: (-far(d, (0, 0)), d)), sides, reach


def kernel(
    sizes,
    p_hbm, u_hbm, v_hbm, w_hbm, s_hbm, thick_hbm, owner_hbm,
    out,
    p, u, v, w, s, part, hs, vs, inv, binv, g, lam, mu, alpha, sig, sig_east, sig_west,
    edge, edge_recv, first_row, row_recv, sig_edge, sig_edge_recv, sig_rows, p_edge, p_rows,
    integ, gath, rim, rim_recv, lip, lip_recv, held, chosen, arrived, thick, owner,
    load_sem, small_sem, send_sem, member_sem, recv_sem, round_sem,
):
    n_mem, n_ty, n_tx = sizes
    own, levels, rows, cols = u.shape
    quarter = rows // n_mem
    body = pl.ds(PAD, rows)
    mem, ty, tx = lax.axis_index("mem"), lax.axis_index("ty"), lax.axis_index("tx")
    me = ty * n_tx + tx
    east, west = lax.rem(tx + 1, n_tx), lax.rem(tx + n_tx - 1, n_tx)
    north, south = lax.rem(ty + 1, n_ty), lax.rem(ty + n_ty - 1, n_ty)
    scope = jax.named_scope

    homes, serve, hops, sides, reach = layout(n_ty, n_tx)

    def shift(*offsets):
        return sum(o[0] for o in offsets) % n_ty, sum(o[1] for o in offsets) % n_tx

    def place(*offsets, **at):
        a, b = shift(*offsets)
        return {"ty": lax.rem(ty + a, n_ty), "tx": lax.rem(tx + b, n_tx), **at}

    def member(i):
        return {"mem": lax.rem(mem + i, n_mem)}

    across, along = [place(o) for o in sides[:2]], [place(o) for o in sides[2:]]
    others = [member(i) for i in range(1, n_mem)]
    rounds = [across + along] * (reach - 1) + [others]

    def greet(sem, peers):
        for where in peers:
            pl.semaphore_signal(sem, inc=1, device_id=where, device_id_type=MESH)

    near = across + along + others
    barrier = pltpu.get_barrier_semaphore()
    greet(barrier, near)
    met = []

    def meet(more):
        for _ in range(more):
            n = len(met)
            if n == 0:
                pl.semaphore_wait(barrier, len(near))
            elif n <= len(rounds):
                pl.semaphore_wait(round_sem.at[n - 1], len(rounds[n - 1]))
            if n < len(rounds):
                greet(round_sem.at[n], rounds[n])
            met.append(n)

    def load(src, dst, sem):
        copy = pltpu.make_async_copy(src, dst, sem)
        copy.start()
        return copy

    loads = {}
    for m in range(own):
        loads["p", m] = load(p_hbm.at[m], p.at[m, :, body, :], load_sem.at[3 * m])
        loads["u", m] = load(u_hbm.at[m], u.at[m], load_sem.at[3 * m + 1])
        loads["v", m] = load(v_hbm.at[m], v.at[m, :, pl.ds(0, rows), :], load_sem.at[3 * m + 2])
        if m == 0:
            small = [load(thick_hbm, thick, small_sem.at[0]), load(owner_hbm, owner, small_sem.at[1])]
            loads["s"] = load(s_hbm, s, load_sem.at[3 * own])
    loads["w"] = load(w_hbm, w, load_sem.at[3 * own + 1])

    lane = lax.broadcasted_iota(jnp.int32, (rows, cols), 1)
    row = lax.broadcasted_iota(jnp.int32, (rows, cols), 0)
    lane8 = lax.broadcasted_iota(jnp.int32, (8, cols), 1)
    row8 = lax.broadcasted_iota(jnp.int32, (8, cols), 0)
    column_of = lane - 8 * lax.rem(row, quarter)
    pair = lane >> 1
    even = (lane & 1) == 0
    is_first, is_last = lane == 0, lane == cols - 1
    is_edge = is_first | is_last
    zero = jnp.zeros((rows, cols), jnp.float32)
    blank = jnp.zeros((1, cols), jnp.float32)

    def to_west(x):
        return pltpu.roll(x, cols - 1, 1)

    def to_east(x):
        return pltpu.roll(x, 1, 1)

    def drain(ref, sem):
        pltpu.make_async_copy(ref, ref, sem).wait()

    def send(src, dst, kind, sem, where):
        pltpu.make_async_remote_copy(
            src_ref=src, dst_ref=dst, send_sem=send_sem.at[kind], recv_sem=sem, device_id=where, device_id_type=MESH
        ).start()

    def clear(k, c):
        for m in range(own):
            p[m, k, PAD - 1 : PAD, :] = blank
            p[m, k, PAD + rows : PAD + rows + 1, :] = blank
            v[m, k, rows : rows + 1, :] = blank
        sig[k, PAD - 1 : PAD, :] = blank
        sig[k, PAD + rows : PAD + rows + 1, :] = blank
        return c

    def pack(m):
        def one(k, packed):
            pk = p[m, k, body, :]
            ends = jnp.where(is_last, pk, u[m, k] - horiz_ratio * pk)
            return jnp.where(pair == k, pltpu.roll(ends, 2 * k + 1, 1), packed)

        edge[m] = unrolled(levels, one, zero, 50)

    def pack_rows(m):
        def one(k, c):
            first_row[m, pl.ds(k, 1), :] = v[m, k, 0:1, :] - horiz_ratio * p[m, k, PAD : PAD + 1, :]
            return c

        unrolled(levels, one, 0, 50)

    def pivots():
        def one(i, c):
            k = i + 1
            below, gprev, mass_below, value = c
            sk = s[k]
            hs[k] = horiz_ratio * sk
            vs[k] = vert_ratio * sk
            b = (vert_ratio * vert_ratio) * sk
            mass = thick[k] * sk
            r = 1.0 / (1.0 + b + below - below * gprev)
            gk = b * r
            bi = below * r
            value = (vert_ratio * (mass - mass_below)) * r + bi * value
            inv[k] = r
            binv[k] = bi
            g[k] = gk
            lam[k] = value
            return b, gk, mass, value

        s0 = s[0]
        hs[0] = horiz_ratio * s0
        vs[0] = vert_ratio * s0
        unrolled(levels - 1, one, ((vert_ratio * vert_ratio) * s0, zero, thick[0] * s0, zero))

    def adjoint():
        def weights(k, here, above, packed, lean):
            mk = thick[k] - vert_ratio * (here - above)
            sk = (horiz_ratio * mk) * hs[k]
            ak = mk - 4.0 * sk
            sig[k, body, :] = sk
            sig_east[k] = to_west(sk)
            sig_west[k] = to_east(sk)
            alpha[k] = ak
            mu[k] = mk + ak
            push = ak * vs[k]
            lam[k + 1] = lean - push
            return jnp.where(pair == k, pltpu.roll(sk, 2 * k + 1, 1), packed), here + push

        def two(i, c):
            k = levels - 1 - i
            above, packed, lean = c
            here = lam[k] + g[k] * above
            return here, *weights(k, here, above, packed, lean)

        above, packed, lean = unrolled(levels - 1, two, (zero, zero, zero), 49)
        sig_edge[...] = weights(0, zero, above, packed, lean)[0]

    def diverge(m):
        def one(k, c):
            usum, vsum, psum, rest = c
            pk, uk, vk = p[m, k, body, :], u[m, k], v[m, k, pl.ds(0, rows), :]
            around = to_east(pk) + (p[m, k, pl.ds(PAD - 1, rows), :] + p[m, k, pl.ds(PAD + 1, rows), :])
            div = (to_west(uk - horiz_ratio * pk) - uk) + (v[m, k, pl.ds(1, rows), :] - vk)
            u[m, k] = div - horiz_ratio * (around - 4.0 * pk)
            tk = thick[k]
            return usum + tk * uk, vsum + tk * vk, psum + tk * pk, rest + alpha[k] * pk

        return unrolled(levels, one, (zero, zero, zero, zero), 50)

    def forward(m, rest):
        mine = edge[m]
        halo = jnp.where(
            even, -horiz_ratio * (edge_recv[m, 0] - mine), pltpu.roll(edge_recv[m, 1] - mine, cols - 2, 1))

        def level(k, rest):
            hk = pltpu.roll(halo, cols - 2 * k if not isinstance(k, int) or k > 0 else 0, 1)
            div = u[m, k] + jnp.where(is_edge, hk, 0.0)
            low = jnp.where(row8 == 0, -horiz_ratio * row_recv[m, 0, pl.ds(k, 1), :], 0.0)
            high = jnp.where(row8 == 7, row_recv[m, 1, pl.ds(k, 1), :], 0.0)
            div = jnp.concatenate([div[:8] + low, div[8 : rows - 8], div[rows - 8 :] + high], axis=0)
            e = hs[k] * div
            pa = p[m, k, body, :] - e
            part[m, k] = pa
            return pa, rest - mu[k] * e

        def one(i, c):
            k = i + 1
            pa_below, value, rest = c
            pa, rest = level(k, rest)
            rhs = w[m, i] - vert_ratio * (pa - pa_below)
            value = rhs * inv[k] + binv[k] * value
            w[m, i] = value
            return pa, value, rest

        pa, rest = level(0, rest)
        return unrolled(levels - 1, one, (pa, zero, rest), 49)[2]

    def backward(m, rest):
        def weigh(k, pk, packed, mass, rest, te, tw, tn, ts):
            p_rows[m, 0, pl.ds(k, 1), :] = pk[0:1]
            p_rows[m, 1, pl.ds(k, 1), :] = pk[rows - 1 : rows]
            return (
                jnp.where(pair == k, pltpu.roll(pk, 2 * k + 1, 1), packed),
                mass + thick[k] * pk,
                rest,
                te + sig_east[k] * pk,
                tw + sig_west[k] * pk,
                tn + sig[k, pl.ds(PAD + 1, rows), :] * pk,
                ts + sig[k, pl.ds(PAD - 1, rows), :] * pk,
            )

        def one(i, c):
            k = levels - 1 - i
            above, packed, mass, rest, *sides = c
            here = w[m, k - 1] + g[k] * above
            pk = part[m, k] - vs[k] * (above - here)
            return (here, *weigh(k, pk, packed, mass, rest + lam[k] * here, *sides))

        above, *sums = unrolled(levels - 1, one, (zero, zero, zero, rest, zero, zero, zero, zero), 49)
        packed, *sums = weigh(0, part[m, 0] - vs[0] * above, *sums)
        p_edge[m] = packed
        return sums

    def whole(m, usum, vsum, q, rest, te, tw, tn, ts):
        total = rest + jnp.where(is_first, 0.0, to_east(te)) + jnp.where(is_last, 0.0, to_west(tw))
        total = total + pltpu.roll(tn, 1, 0) + pltpu.roll(ts, rows - 1, 0)
        ue = usum - horiz_ratio * (q - jnp.where(is_first, 0.0, to_east(q)))
        vn = vsum - horiz_ratio * (q - jnp.where(row == 0, 0.0, pltpu.roll(q, 1, 0)))
        for r in range(n_mem):
            for f, x in enumerate((total, ue, vn)):
                integ[m, r, f] = x[r * quarter : (r + 1) * quarter]

    def send_whole(m):
        for n, h in reversed(list(enumerate(homes))):
            for i in range(0 if n else 1, n_mem):
                other = lax.rem(mem + i, n_mem)
                send(integ.at[m, other], gath.at[n * n_mem + mem, m], 4, recv_sem.at[2], place(h, mem=other))

    def rims(qs):
        sig_e, sig_w = pltpu.roll(sig_edge_recv[1], cols - 1, 1), pltpu.roll(sig_edge_recv[0], 1, 1)
        rims = zero
        for m in range(own):
            te = jnp.sum(jnp.where(even, sig_e * p_edge[m], 0.0), axis=1, keepdims=True)
            tw = jnp.sum(jnp.where(even, 0.0, sig_w * p_edge[m]), axis=1, keepdims=True)
            q = jnp.sum(jnp.where(is_last, qs[m], 0.0), axis=1, keepdims=True)
            for c, x in ((2 * m, te), (2 * m + 1, q), (2 * own + m, tw)):
                rims = jnp.where(column_of == c, x, rims)
        for r in range(n_mem):
            rim[r] = jnp.sum(rims[r * quarter : (r + 1) * quarter], axis=0, keepdims=True)

    def send_rims():
        for n, h in reversed(list(enumerate(homes))):
            for goal in sorted(range(n_mem), key=lambda q: (q % 2, q)):
                for kind in range(2):
                    send(
                        rim.at[goal], rim_recv.at[n, kind, mem], 5, recv_sem.at[3],
                        place(h, sides[kind], mem=goal))

    def lips(qs):
        for m in range(own):
            lip[m : m + 1, :] = jnp.sum(sig_rows[0] * p_rows[m, 1], axis=0, keepdims=True)
            lip[own + m : own + m + 1, :] = qs[m][rows - 1 : rows]
            lip[2 * own + m : 2 * own + m + 1, :] = jnp.sum(sig_rows[1] * p_rows[m, 0], axis=0, keepdims=True)

    goals = (0, n_mem - 1)
    kept = [sum(shift(h, sides[2 + kind]) == (0, 0) for h in homes) for kind in range(2)]

    def send_lips():
        for n, h in reversed(list(enumerate(homes))):
            for kind, goal in enumerate(goals):
                at = n * n_mem + mem
                if shift(h, sides[2 + kind]) != (0, 0):
                    send(lip, lip_recv.at[kind, at], 6, recv_sem.at[4], place(h, sides[2 + kind], mem=goal))
                    continue

                @pl.when(mem != goal)
                def _():
                    send(lip, lip_recv.at[kind, at], 8 + kind, recv_sem.at[4], {"mem": goal})

                @pl.when(mem == goal)
                def _():
                    lip_recv[kind, at] = lip[...]

    with scope("clear"):
        unrolled(levels, clear, 0, 10)
    for m in range(own):
        with scope(f"wait_p{m}"):
            loads["p", m].wait()
        with scope(f"wait_u{m}"):
            loads["u", m].wait()
        with scope(f"pack{m}"):
            pack(m)
        if m == 0:
            with scope("wait_barrier"):
                meet(1)
        with scope(f"send{m}"):
            send(p.at[m, :, PAD + rows - 1, :], row_recv.at[m, 0], 0, member_sem.at[m, 0], {"ty": north})
            send(edge.at[m], edge_recv.at[m, 0], 1, member_sem.at[m, 1], {"tx": east})
            send(edge.at[m], edge_recv.at[m, 1], 1, member_sem.at[m, 1], {"tx": west})
        with scope(f"wait_v{m}"):
            loads["v", m].wait()
        with scope(f"rows{m}"):
            pack_rows(m)
            send(first_row.at[m], row_recv.at[m, 1], 0, member_sem.at[m, 0], {"ty": south})
        if m == 0:
            with scope("wait_s"):
                loads["s"].wait()
                for copy in small:
                    copy.wait()
            with scope("pivots"):
                pivots()
    with scope("adjoint"):
        adjoint()
    with scope("send_sig"):
        send(sig_edge, sig_edge_recv.at[0], 2, recv_sem.at[0], {"tx": east})
        send(sig_edge, sig_edge_recv.at[1], 2, recv_sem.at[0], {"tx": west})
        send(sig.at[:, PAD, :], sig_rows.at[0], 3, recv_sem.at[1], {"ty": south})
        send(sig.at[:, PAD + rows - 1, :], sig_rows.at[1], 3, recv_sem.at[1], {"ty": north})
    sums = []
    for m in range(own):
        with scope(f"diverge{m}"):
            sums.append(diverge(m))
        if m == 0:
            with scope("meet0"):
                meet(len(rounds) - 1)

    qs = []
    for m in range(own):
        with scope(f"wait_edge{m}"):
            if m == 0:
                loads["w"].wait()
            drain(edge_recv.at[m], member_sem.at[m, 1])
        with scope(f"wait_row{m}"):
            drain(row_recv.at[m], member_sem.at[m, 0])
        with scope(f"forward{m}"):
            rest = forward(m, sums[m][3])
        with scope(f"backward{m}"):
            mass, *rest = backward(m, rest)
        qs.append(sums[m][2] + mass)
        last = m == own - 1
        if m == 0:
            with scope("meet"):
                meet(len(rounds) + 1 - len(met))
        if last:
            with scope("wait_sig"):
                drain(sig_edge_recv, recv_sem.at[0])
                drain(sig_rows, recv_sem.at[1])
        with scope(f"sums{m}"):
            if last:
                rims(qs)
                send_rims()
                lips(qs)
            whole(m, sums[m][0], sums[m][1], qs[m], *rest)
        with scope(f"send_sums{m}"):
            if last:
                send_lips()
            send_whole(m)

    bottom = (row8[:quarter] == 0) & (mem == 0)
    top = (row8[:quarter] == quarter - 1) & (mem == n_mem - 1)
    with scope("wait_lip"):

        for kind, goal in enumerate(goals):

            @pl.when(mem == goal)
            def _():
                drain(lip_recv.at[kind, pl.ds(0, len(homes) * n_mem - kept[kind])], recv_sem.at[4])

    with scope("wait_rim"):
        drain(rim_recv, recv_sem.at[3])
    with scope("wait_mem"):
        drain(gath.at[pl.ds(0, len(homes) * n_mem - 1)], recv_sem.at[2])

    lane_q = lane[:quarter]

    def column(x, c):
        return jnp.sum(jnp.where(column_of[:quarter] == c, x, 0.0), axis=1, keepdims=True)

    def stats(n):
        fields = []
        for i in range(n_mem):
            other = lax.rem(mem + i, n_mem)
            from_west, from_east = rim_recv[n, 0, other], rim_recv[n, 1, other]
            from_south, from_north = lip_recv[0, n * n_mem + other], lip_recv[1, n * n_mem + other]
            for m in range(own):
                source = integ.at[m, mem] if n == 0 and i == 0 else gath.at[n * n_mem + other, m]
                total, ue, vn = (source[f] for f in range(3))
                te, qw = column(from_west, 2 * m), column(from_west, 2 * m + 1)
                tw = column(from_east, 2 * own + m)
                total = total + jnp.where(lane_q == 0, te, 0.0) + jnp.where(lane_q == cols - 1, tw, 0.0)
                total = total + jnp.where(bottom, from_south[m : m + 1], 0.0)
                total = total + jnp.where(top, from_north[2 * own + m : 2 * own + m + 1], 0.0)
                ue = ue + horiz_ratio * jnp.where(lane_q == 0, qw, 0.0)
                vn = vn + horiz_ratio * jnp.where(bottom, from_south[own + m : own + m + 1], 0.0)
                fields.append([total, ue, vn])

        members = len(fields)
        for f in range(3):
            total = fields[0][f]
            for one in fields[1:]:
                total = total + one[f]
            mean = total / members
            second = (fields[0][f] - mean) ** 2
            for one in fields[1:]:
                second = second + (one[f] - mean) ** 2
            held[n, f] = mean
            held[n, 3 + f] = second / (members - 1)

    def number(o):
        where = place(o)
        return where["ty"] * n_tx + where["tx"]

    def back(o):
        return (-o[0] % n_ty, -o[1] % n_tx)

    with scope("stats"):
        for n in range(len(homes)):
            stats(n)
        for i, hop in enumerate(hops):
            pick = jnp.int32(0)
            for n, h in enumerate(homes):
                if serve[shift(hop, h)] == n:
                    pick = jnp.where(owner[number(back(h))] == number(hop), n, pick)
            chosen[i] = held[pick]
            send(chosen.at[i], arrived.at[i], 7, recv_sem.at[5], place(hop))
        here, there, local = jnp.int32(0), jnp.int32(0), jnp.int32(0)
        for o, n in serve.items():
            found = owner[number(back(o))] == me
            hop = shift(o, back(homes[n]))
            if hop == (0, 0):
                here = jnp.where(found, n, here)
                local = jnp.where(found, 1, local)
            else:
                there = jnp.where(found, hops.index(hop), there)
    with scope("wait_all"):
        drain(arrived, recv_sem.at[5])
    with scope("finish"):
        out[0, 0] = jnp.where(local == 1, held[here], arrived[there])
        drain(row_recv, send_sem.at[0])
        drain(edge_recv, send_sem.at[1])
        drain(sig_edge_recv, send_sem.at[2])
        drain(sig_rows, send_sem.at[3])
        drain(gath.at[pl.ds(0, len(homes) * n_mem - 1)], send_sem.at[4])
        drain(rim_recv, send_sem.at[5])
        drain(lip_recv.at[0, pl.ds(0, 2 * len(homes) - kept[0] - kept[1])], send_sem.at[6])
        for kind, goal in enumerate(goals):
            if kept[kind]:

                @pl.when(mem != goal)
                def _():
                    drain(lip_recv.at[0, pl.ds(0, kept[kind])], send_sem.at[8 + kind])

        drain(arrived, send_sem.at[7])


def solution(mesh):
    n_mem, n_ty, n_tx = (mesh.shape[a] for a in ("mem", "ty", "tx"))
    homes, _, hops, _, reach = layout(n_ty, n_tx)

    def local(pressure, east_wind, north_wind, vertical_wind, sound_squared, thickness, owner_map):
        own, levels, rows, cols = pressure.shape
        quarter = rows // n_mem
        f32 = jnp.float32
        dma = pltpu.SemaphoreType.DMA

        def vmem(*shape):
            return pltpu.VMEM(shape, f32)

        return pl.pallas_call(
            functools.partial(kernel, (n_mem, n_ty, n_tx)),
            name="acoustic",
            out_shape=pltpu.VMEM((1, 1, 6, quarter, cols), f32),
            in_specs=[pl.BlockSpec(memory_space=pl.ANY)] * 7,
            out_specs=pl.BlockSpec(memory_space=pltpu.VMEM),
            scratch_shapes=[
                vmem(own, levels, rows + 2 * PAD, cols),
                vmem(own, levels, rows, cols),
                vmem(own, levels, rows + PAD, cols),
                vmem(own, levels - 1, rows, cols),
                vmem(levels, rows, cols),
                vmem(own, levels, rows, cols),
                *[vmem(levels + 1, rows, cols)] * 8,
                vmem(levels, rows + 2 * PAD, cols),
                *[vmem(levels, rows, cols)] * 2,
                vmem(own, rows, cols),
                vmem(own, 2, rows, cols),
                vmem(own, levels, cols),
                vmem(own, 2, levels, cols),
                vmem(rows, cols),
                vmem(2, rows, cols),
                vmem(2, levels, cols),
                vmem(own, rows, cols),
                vmem(own, 2, levels, cols),
                vmem(own, n_mem, 3, quarter, cols),
                vmem(len(homes) * n_mem, own, 3, quarter, cols),
                vmem(n_mem, 1, cols),
                vmem(len(homes), 2, n_mem, 1, cols),
                vmem(-(-3 * own // 8) * 8, cols),
                vmem(2, len(homes) * n_mem, -(-3 * own // 8) * 8, cols),
                vmem(len(homes), 6, quarter, cols),
                vmem(len(hops), 6, quarter, cols),
                vmem(len(hops), 6, quarter, cols),
                pltpu.SMEM(thickness.shape, f32),
                pltpu.SMEM(owner_map.shape, jnp.int32),
                dma((3 * own + 2,)),
                dma((2,)),
                dma((10,)),
                dma((own, 2)),
                dma((6,)),
                pltpu.SemaphoreType.REGULAR((reach,)),
            ],
            compiler_params=pltpu.CompilerParams(collective_id=0, has_side_effects=True),
        )(pressure, east_wind, north_wind, vertical_wind, sound_squared, thickness, owner_map)

    field = P("mem", None, "ty", "tx")
    return jax.shard_map(
        local,
        mesh=mesh,
        in_specs=(field, field, field, field, P(None, "ty", "tx"), P(), P()),
        out_specs=P("ty", "tx", None, "mem", None),
        check_vma=False,
    )
```
